512 devices in a mesh: gx: 8 (over z), gy: 8 (over y_lo, x), gz: 8 (over y_hi, core).
Axes of the slice: x: 4, y: 8 (y_hi: 4, y_lo: 2; y = y_hi * 2 + y_lo), z: 8, core: 2. Of those that a mesh axis runs over, the one named last changes fastest.
Arguments:
- orbitals: bfloat16 [8, 256, 65536], P(None, 'gx', ('gy', 'gz')), may hold values from -6 to 6
- potential: float32 [128, 128, 128], P('gx', 'gy', 'gz'), may hold values from -3 to 0
- ion_potential: float32 [128, 128, 128], P('gx', 'gy', 'gz'), may hold values from -2 to 0
- occupations: float32 [8], replicated, may hold values from 0.005 to 0.08
Outputs:
- new_orbitals: bfloat16 [8, 256, 65536], P(None, 'gx', ('gy', 'gz'))
- density: float32 [128, 128, 128], P('gx', 'gy', 'gz')
- new_potential: float32 [256, 65536], P('gx', ('gy', 'gz'))
The draws below stay inside these ranges and needn't reach their ends.
All inputs are finite; a program needn't handle non-finite values.
Results may differ from the reference program's by a relative error of at most 0.001.
Values sent between devices are 32-bit elements; how exact they have to be, the bound alone decides.
No kernel may reach another device: no remote copies, remote signals or barrier semaphores. Data moves between devices by JAX's collectives and lax.ppermute only.
A program may use at most 64 MiB of HBM per device.

```python
import math
import jax
import jax.numpy as jnp
from jax import lax

CORE = 16
BUF = 8
NORB = 8
DEGREE = 10
LX = 32
NX = 128
NY = 128
NZ = 128
N_GX = 8
N_GY = 8
N_GZ = 8


def steps_of(rng, dims, shards, least, largest):
    def one(dim, blocks):
        heights = jax.random.uniform(jax.random.fold_in(jax.random.fold_in(rng, 6), dim), (blocks,), jnp.float32, least / len(shards), largest / len(shards))
        return jnp.repeat(jnp.exp(heights), dims[dim] // blocks).reshape((-1,) + (1,) * (len(dims) - dim - 1))

    level = one(*shards[0])
    for cut in shards[1:]:
        level = level * one(*cut)
    return level


def bell_draw(key, shape, deviation, limit, cuts=(), kind=jnp.bfloat16):
    values = jax.random.normal(key, shape, jnp.float32) * deviation
    if len(cuts) > 0:
        values = steps_of(key, shape, cuts, -0.22, 0.18) * values
    return jnp.clip(values, min=-limit, max=limit).astype(kind)


def setup_inputs(seed: int = 0) -> dict:
    streams_of = jax.random.split(jax.random.key(seed), 5)
    return {
        "orbitals": bell_draw(streams_of[0], (NORB, N_GX * LX, N_GY * N_GZ * LX * LX), 1.0, 6.0, ((1, 8), (2, 64))),
        "potential": jnp.clip(-3.0 + 3.0 * jax.random.uniform(streams_of[1], (NX, NY, NZ), jnp.float32) ** steps_of(streams_of[1], (NX, NY, NZ), ((0, 8), (1, 8), (2, 8)), -0.2, 0.2), -3.0, 0.0),
        "ion_potential": jnp.clip(-2.0 + 2.0 * jax.random.uniform(streams_of[2], (NX, NY, NZ), jnp.float32) ** steps_of(streams_of[2], (NX, NY, NZ), ((0, 8), (1, 8), (2, 8)), -0.2, 0.2), -2.0, 0.0),
        "occupations": jnp.clip(jnp.exp(jax.random.uniform(streams_of[3], (NORB,), jnp.float32, math.log(0.005), math.log(0.08))), 0.005, 0.08),
    }


spacing = 0.2
kinetic = 0.5 / (spacing * spacing)
filter_low = 6.0
filter_high = 12.0 * kinetic
centre_value = 0.5 * (filter_low + filter_high)
half_width = 0.5 * (filter_high - filter_low)

def hamiltonian(vectors, potential_ext, edge_len):
    extent = vectors.shape[2]
    padded = jnp.pad(vectors, ((0, 0), (1, 1), (0, 0)))
    beside = padded[:, 2:] + padded[:, :-2]
    padded = jnp.pad(vectors, ((0, 0), (0, 0), (edge_len, edge_len)))
    beside = beside + padded[:, :, 2 * edge_len:] + padded[:, :, :-2 * edge_len]
    padded = jnp.pad(vectors, ((0, 0), (0, 0), (1, 1)))
    column = jnp.arange(extent, dtype=jnp.int32) % edge_len
    up_mask = (column < edge_len - 1).astype(vectors.dtype)
    down_mask = (column > 0).astype(vectors.dtype)
    beside = beside + padded[:, :, 2:] * up_mask + padded[:, :, :-2] * down_mask
    return -kinetic * (beside - 6.0 * vectors) + potential_ext * vectors

def chebyshev(initial, potential_ext, edge_len):
    leading = (hamiltonian(initial, potential_ext, edge_len) - centre_value * initial) / half_width

    def advance(counter, states):
        previous, current = states
        following = 2.0 * (hamiltonian(current, potential_ext, edge_len) - centre_value * current) / half_width - previous
        return (current, following)
    return lax.fori_loop(1, DEGREE, advance, (initial, leading))[1]

def orthonormal(filtered):
    orbital_count = filtered.shape[0]
    flattened = filtered.reshape(orbital_count, -1)
    intersection = jnp.dot(flattened, flattened.T, precision=lax.Precision.HIGHEST) / flattened.shape[1]
    factor = jnp.linalg.cholesky(intersection)
    identity = jnp.eye(orbital_count, dtype=filtered.dtype)
    inverse = lax.linalg.triangular_solve(factor, identity, left_side=True, lower=True)
    return jnp.dot(inverse, flattened, precision=lax.Precision.HIGHEST).reshape(filtered.shape)

def ramp(extent):
    position = jnp.arange(extent, dtype=jnp.float32)
    rising = jnp.clip((position + 0.5 - 0.5 * BUF) / BUF, 0.0, 1.0)
    falling = jnp.clip((extent - 0.5 * BUF - 0.5 - position) / BUF, 0.0, 1.0)
    return rising * falling

def window_weight(edge_len):
    profile = ramp(edge_len)
    return profile[:, None] * (profile[:, None] * profile[None, :]).reshape(1, edge_len * edge_len)

def exchange_correlation(density):
    cube_root = jnp.cbrt(density)
    slater = -(3.0 / math.pi) ** (1.0 / 3.0) * cube_root
    radius = (3.0 / (4.0 * math.pi)) ** (1.0 / 3.0)
    bottom = radius + 7.8 * cube_root
    wigner = -0.44 * cube_root / bottom * (1.0 + radius / (3.0 * bottom))
    return slater + wigner

def wave_term(extent, initial, period):
    indices = (initial + jnp.arange(extent, dtype=jnp.int32)).astype(jnp.float32)
    return 4.0 / (spacing * spacing) * jnp.sin(math.pi * indices / period) ** 2

def kernel(extents, starts, periods):
    eigen_sum = wave_term(extents[0], starts[0], periods[0])[:, None, None] + wave_term(extents[1], starts[1], periods[1])[None, :, None] + wave_term(extents[2], starts[2], periods[2])[None, None, :]
    positive = eigen_sum > 0.0
    return jnp.where(positive, 4.0 * math.pi / jnp.where(positive, eigen_sum, 1.0), 0.0)

def offsets(count):
    return jnp.arange(count, dtype=jnp.int32)[:, None] * CORE + jnp.arange(LX, dtype=jnp.int32)[None, :]

def windows(field):
    padded = jnp.pad(field, BUF, mode='wrap')
    picked = jnp.take(padded, offsets(N_GX), axis=0)
    picked = jnp.take(picked, offsets(N_GY), axis=2)
    return jnp.take(picked, offsets(N_GZ), axis=4)

def fold_axis(values, dom_axis, loc_axis):
    low_rows = lax.slice_in_dim(values, 0, BUF, axis=loc_axis)
    interior = lax.slice_in_dim(values, BUF, BUF + CORE, axis=loc_axis)
    high_rows = lax.slice_in_dim(values, BUF + CORE, LX, axis=loc_axis)
    pad_low = [(0, 0)] * values.ndim
    pad_low[loc_axis] = (CORE - BUF, 0)
    pad_high = [(0, 0)] * values.ndim
    pad_high[loc_axis] = (0, CORE - BUF)
    return interior + jnp.pad(jnp.roll(low_rows, -1, axis=dom_axis), pad_low) + jnp.pad(jnp.roll(high_rows, 1, axis=dom_axis), pad_high)

def reference(orbitals, potential, ion_potential, occupations):
    domains = N_GX * N_GY * N_GZ
    plane_cells = LX * LX
    stacked = orbitals.reshape(NORB, N_GX, LX, N_GY * N_GZ, plane_cells).transpose(1, 3, 0, 2, 4)
    stacked = stacked.reshape(domains, NORB, LX, plane_cells)
    fields = windows(potential).transpose(0, 2, 4, 1, 3, 5).reshape(domains, LX, plane_cells)
    weight = window_weight(LX)

    def domain_work(states):
        initial, potential_ext = states
        filtered = chebyshev(initial.astype(jnp.float32), potential_ext, LX)
        normal_set = orthonormal(filtered)
        partial_value = weight * jnp.sum(occupations[:, None, None] * normal_set * normal_set, axis=0)
        return (normal_set.astype(jnp.bfloat16), partial_value)
    new_stack, partials = lax.map(domain_work, (stacked, fields))
    new_orbitals = new_stack.reshape(N_GX, N_GY * N_GZ, NORB, LX, plane_cells).transpose(2, 0, 3, 1, 4)
    new_orbitals = new_orbitals.reshape(NORB, N_GX * LX, N_GY * N_GZ * plane_cells)
    values = partials.reshape(N_GX, N_GY, N_GZ, LX, LX, LX)
    values = fold_axis(values, 0, 3)
    values = fold_axis(values, 1, 4)
    values = fold_axis(values, 2, 5)
    density = values.transpose(0, 3, 1, 4, 2, 5).reshape(NX, NY, NZ)
    kernel_grid = kernel((NX, NY, NZ), (0, 0, 0), (NX, NY, NZ))
    hartree = jnp.real(jnp.fft.ifftn(jnp.fft.fftn(density) * kernel_grid)).astype(density.dtype)
    interior = ion_potential + hartree + exchange_correlation(density)
    new_potential = windows(interior).transpose(0, 1, 2, 4, 3, 5).reshape(N_GX * LX, N_GY * N_GZ * plane_cells)
    return (new_orbitals, density, new_potential)
```

```python
import functools
import math

import jax
import jax.numpy as jnp
import numpy as np
from jax import lax
from jax.experimental import pallas as pl
from jax.experimental.pallas import tpu as pltpu
from jax.sharding import PartitionSpec as P

BUF = 8
DEGREE = 10
N = 128
CORE = 16
LX = 32
NORB = 8
PARTS = 8
FIRST, LAST = 4, 28
KEPT = LAST - FIRST
LANES = 128
PER = LANES // LX

spacing = 0.2
kinetic = 0.5 / (spacing * spacing)
filter_low = 6.0
filter_high = 12.0 * kinetic
centre_value = 0.5 * (filter_low + filter_high)
half_width = 0.5 * (filter_high - filter_low)

F32, BF16 = jnp.float32, jnp.bfloat16
VMEM = pl.BlockSpec(memory_space=pltpu.VMEM)
SMEM = pl.BlockSpec(memory_space=pltpu.SMEM)
INTERPRET = False


def call(kernel, out_shape, in_specs, scratch=(), flops=1000000, name=None):
    many = isinstance(out_shape, (tuple, list))
    return pl.pallas_call(
        kernel,
        out_shape=out_shape,
        in_specs=in_specs,
        out_specs=tuple(VMEM for _ in out_shape) if many else VMEM,
        scratch_shapes=scratch,
        compiler_params=pltpu.CompilerParams(vmem_limit_bytes=40 * 1024 * 1024),
        cost_estimate=pl.CostEstimate(flops=flops, bytes_accessed=1000000, transcendentals=0),
        interpret=INTERPRET,
        name=name,
    )


def _basis():
    n = np.arange(N, dtype=np.float64)
    angle = 2.0 * np.pi * np.mod(np.outer(n, n), N) / N
    return (np.cos(angle) + np.sin(angle)) / math.sqrt(N)


def _pair(table):
    high = np.asarray(table, np.float32).astype(jnp.bfloat16)
    low = (np.asarray(table, np.float64) - high.astype(np.float64)).astype(jnp.bfloat16)
    return high, low


def _cell(part, a):
    return np.mod(CORE * part + a - BUF, N)


def _tables():
    basis = _basis()
    parts = np.arange(PARTS)
    along = np.zeros((PARTS, CORE + LX, PARTS * KEPT))
    for i in range(PARTS):
        for other in range(PARTS):
            for xx in range(KEPT):
                column = other * KEPT + xx
                cell = _cell(other, xx + FIRST)
                along[i, :CORE, column] = basis[CORE * i : CORE * (i + 1), cell]
                for a in range(LX):
                    if _cell(i, a) == cell and min((other - i) % PARTS, (i - other) % PARTS) <= 1:
                        along[i, CORE + a, column] = 1.0
    lane = np.arange(PARTS * LANES)
    z_cell = _cell(lane // LANES, lane % LX)
    z_table = basis[z_cell, :]
    y_lo, y_hi, j = np.meshgrid(np.arange(PER), np.arange(KEPT // PER), parts, indexing="ij")
    y_table = basis[:, _cell(j, FIRST + PER * y_hi + y_lo).reshape(-1)]
    back = np.zeros((4, 64, N))
    for q in range(4):
        y_lo, y_half, j = np.meshgrid(np.arange(PER), np.arange(2), parts, indexing="ij")
        back[q] = basis[_cell(j, 8 * q + PER * y_half + y_lo).reshape(-1), :]
    last = np.stack([basis[_cell(i, np.arange(LX)), :] for i in range(PARTS)])
    wave = 4.0 / (spacing * spacing) * np.sin(np.pi * np.arange(N) / N) ** 2
    return dict(
        along=_pair(along),
        z_table=_pair(z_table),
        z_back=_pair(z_table.T),
        y_table=_pair(y_table),
        y_back=_pair(back),
        last=_pair(last),
        wave=wave.astype(np.float32),
        wave_yz=(wave[:, None] + wave[None, :]).astype(np.float32),
    )


def _weight():
    position = np.arange(LX, dtype=np.float32)
    rising = np.clip((position + 0.5 - 0.5 * BUF) / BUF, 0.0, 1.0)
    falling = np.clip((LX - 0.5 * BUF - 0.5 - position) / BUF, 0.0, 1.0)
    profile = (rising * falling).astype(np.float32)
    return profile[:, None] * (profile[:, None] * profile[None, :]).reshape(1, LX * LX)


TABLES = _tables()
WEIGHT = _weight().astype(np.float32)


def halves(value):
    high = value.astype(BF16)
    return high, (value - high.astype(F32)).astype(BF16)


def dot3(left, right):
    def one(a, b):
        return jnp.dot(a, b, preferred_element_type=F32)

    return one(left[0], right[0]) + (one(left[0], right[1]) + one(left[1], right[0]))


def iota(shape, dim):
    return lax.broadcasted_iota(jnp.int32, shape, dim)


def filter_kernel(occ_ref, orb_ref, pot_ref, weight_ref, new_ref, send_ref, ya, yb, coef, dens):
    tiles, chunks = LX // 8, LX * LX // LANES
    lane = iota((8, LANES), 1)
    row = iota((8, LANES), 0)
    low_z, high_z = lane % LX == 0, lane % LX == LX - 1
    first_y, last_y = lane < LX, lane >= LANES - LX
    first_x, last_x = row == 0, row == 7
    zero = jnp.zeros((8, LANES), F32)

    coef[...] = (2.0 / half_width) * pot_ref[...] + (2.0 / half_width) * (
        6.0 * kinetic - centre_value
    )
    alpha = -2.0 * kinetic / half_width

    def fill(n, carry):
        for buffer in (ya, yb):
            buffer[n, 0:8, :] = jnp.zeros((8, (chunks + 2) * LANES), F32)
            buffer[n, 8 + LX : 16 + LX, :] = jnp.zeros((8, (chunks + 2) * LANES), F32)
            buffer[n, :, 0:LANES] = jnp.zeros((16 + LX, LANES), F32)
            buffer[n, :, (chunks + 1) * LANES :] = jnp.zeros((16 + LX, LANES), F32)
        ya[n, 8 : 8 + LX, LANES : (chunks + 1) * LANES] = orb_ref[n].astype(F32)
        return carry

    lax.fori_loop(0, NORB, fill, 0)

    def advance(src, dst, start):
        def one(n, carry):
            for c in range(chunks):
                here = slice((c + 1) * LANES, (c + 2) * LANES)
                for t in range(tiles):
                    rows = slice(8 + 8 * t, 16 + 8 * t)
                    cur = src[n, rows, here]
                    above = src[n, 8 * t : 8 + 8 * t, here]
                    below = src[n, 16 + 8 * t : 24 + 8 * t, here]
                    before = src[n, rows, c * LANES : (c + 1) * LANES]
                    after = src[n, rows, (c + 2) * LANES : (c + 3) * LANES]
                    total = pltpu.roll(jnp.where(last_x, above, cur), 1, 0)
                    total += pltpu.roll(jnp.where(first_x, below, cur), 7, 0)
                    total += pltpu.roll(jnp.where(last_y, before, cur), LX, 1)
                    total += pltpu.roll(jnp.where(first_y, after, cur), LANES - LX, 1)
                    total += jnp.where(low_z, zero, pltpu.roll(cur, 1, 1))
                    total += jnp.where(high_z, zero, pltpu.roll(cur, LANES - 1, 1))
                    w = coef[8 * t : 8 + 8 * t, c * LANES : (c + 1) * LANES]
                    result = alpha * total + w * cur
                    if start:
                        dst[n, rows, here] = 0.5 * result
                    else:
                        dst[n, rows, here] = result - dst[n, rows, here]
            return carry

        lax.fori_loop(0, NORB, one, 0)

    advance(ya, yb, True)

    def two(m, carry):
        advance(yb, ya, False)
        advance(ya, yb, False)
        return carry

    lax.fori_loop(0, (DEGREE - 2) // 2, two, 0)
    advance(yb, ya, False)

    pairs = [(n, m) for n in range(NORB) for m in range(n + 1)]

    def gather(t, sums):
        sums = list(sums)
        start = pl.multiple_of(8 + 8 * t, 8)
        for c in range(chunks):
            f = [ya[n, pl.ds(start, 8), (c + 1) * LANES : (c + 2) * LANES] for n in range(NORB)]
            for at, (n, m) in enumerate(pairs):
                sums[at] = sums[at] + f[n] * f[m]
        return tuple(sums)

    sums = lax.fori_loop(0, tiles, gather, tuple(zero for _ in pairs))
    gram = {
        pair: jnp.sum(jnp.sum(s, axis=0, keepdims=True), axis=1, keepdims=True) / float(LX**3)
        for pair, s in zip(pairs, sums)
    }
    factor, inverse, recip = {}, {}, {}
    for j in range(NORB):
        rest = gram[j, j]
        for k in range(j):
            rest = rest - factor[j, k] * factor[j, k]
        recip[j] = 1.0 / jnp.sqrt(rest)
        for n in range(j + 1, NORB):
            value = gram[n, j]
            for k in range(j):
                value = value - factor[n, k] * factor[j, k]
            factor[n, j] = value * recip[j]
    for j in range(NORB):
        inverse[j, j] = recip[j]
        for n in range(j + 1, NORB):
            value = factor[n, j] * inverse[j, j]
            for k in range(j + 1, n):
                value = value + factor[n, k] * inverse[k, j]
            inverse[n, j] = -recip[n] * value
    wide = {pair: jnp.broadcast_to(inverse[pair], (8, LANES)) for pair in pairs}

    def normal(t, carry):
        start = pl.multiple_of(8 + 8 * t, 8)
        rows = pl.ds(pl.multiple_of(8 * t, 8), 8)
        for c in range(chunks):
            here = slice((c + 1) * LANES, (c + 2) * LANES)
            f = [ya[n, pl.ds(start, 8), here] for n in range(NORB)]
            total = zero
            for n in range(NORB):
                value = wide[n, 0] * f[0]
                for m in range(1, n + 1):
                    value = value + wide[n, m] * f[m]
                yb[n, pl.ds(start, 8), here] = value
                total = total + occ_ref[n] * (value * value)
            there = slice(c * LANES, (c + 1) * LANES)
            dens[rows, there] = total * weight_ref[rows, there]
        return carry

    lax.fori_loop(0, tiles, normal, 0)

    def finish(n, carry):
        new_ref[n] = yb[n, 8 : 8 + LX, LANES : (chunks + 1) * LANES].astype(BF16)
        return carry

    lax.fori_loop(0, NORB, finish, 0)

    kept = KEPT // PER
    for c in range(kept):
        value = dens[FIRST:LAST, (c + 1) * LANES : (c + 2) * LANES]
        for s in range(PARTS):
            send_ref[pl.ds(s * KEPT * kept + c, KEPT, stride=kept), :] = value


def filtered_set(occupations, orbitals, potential_ext):
    wide = LX * LX + 2 * LANES
    return call(
        filter_kernel,
        (
            jax.ShapeDtypeStruct((NORB, LX, LX * LX), BF16),
            jax.ShapeDtypeStruct((PARTS * KEPT * KEPT // PER, LANES), F32),
        ),
        [SMEM, VMEM, VMEM, VMEM],
        [
            pltpu.VMEM((NORB, LX + 16, wide), F32),
            pltpu.VMEM((NORB, LX + 16, wide), F32),
            pltpu.VMEM((LX, LX * LX), F32),
            pltpu.VMEM((LX, LX * LX), F32),
        ],
        flops=60000000,
        name="filter",
    )(occupations, orbitals, potential_ext, jnp.asarray(WEIGHT))


def x_kernel(place_ref, got_ref, high_ref, low_ref, send_ref):
    kept = KEPT // PER
    at = place_ref[0]
    table = (high_ref[at], low_ref[at])
    for c in range(kept):
        lines = got_ref[pl.ds(c, PARTS * KEPT, stride=kept), :]
        value = dot3(table, halves(lines))
        for q in range(2):
            send_ref[pl.ds(q * 2 * kept + c, LX, stride=4 * kept), :] = value[CORE:]
        for q in range(4):
            send_ref[pl.ds(q * 2 * kept + kept + c, CORE, stride=8 * kept), :] = value[:CORE]


def along_x(place, got):
    return call(
        x_kernel,
        jax.ShapeDtypeStruct((64 * 2 * KEPT // PER, LANES), F32),
        [SMEM, VMEM, VMEM, VMEM],
        name="along_x",
    )(place, got, *map(jnp.asarray, TABLES["along"]))


def plane_kernel(
    place_ref,
    lx_ref,
    got_ref,
    zh_ref,
    zl_ref,
    yh_ref,
    yl_ref,
    wave_ref,
    bh_ref,
    bl_ref,
    th_ref,
    tl_ref,
    send_ref,
    work,
):
    kept = KEPT // PER
    chunk = 2 * kept
    out_chunk = 6
    wide = PARTS * LANES
    blocks = []
    for k in range(PARTS):
        rows = [
            got_ref[pl.ds(chunk * k + kept + c, PARTS, stride=chunk * PARTS), :]
            for c in range(kept)
        ]
        blocks.append(jnp.concatenate(rows, axis=0))
    lines = jnp.concatenate(blocks, axis=1)
    which = (iota(lines.shape, 1) % LANES) // LX
    spread = jnp.concatenate([jnp.where(which == y, lines, 0.0) for y in range(PER)], axis=0)
    along_z = dot3(halves(spread), (zh_ref[...], zl_ref[...]))
    spectrum = dot3((yh_ref[...], yl_ref[...]), halves(along_z))
    eigen = wave_ref[...] + lx_ref[0]
    positive = eigen > 0.0
    green = jnp.where(positive, 4.0 * math.pi / jnp.where(positive, eigen, 1.0), 0.0)
    spectrum = spectrum * green
    quarter = place_ref[1]
    lines = dot3((bh_ref[quarter], bl_ref[quarter]), halves(spectrum))
    spread = dot3(halves(lines), (th_ref[...], tl_ref[...]))
    which = (iota((16, wide), 1) % LANES) // LX
    packed = jnp.zeros((16, wide), F32)
    for y in range(PER):
        packed = jnp.where(which == y, spread[16 * y : 16 * (y + 1)], packed)
    for k in range(PARTS):
        for half in range(2):
            send_ref[pl.ds(out_chunk * k + half, PARTS, stride=out_chunk * PARTS), :] = packed[
                8 * half : 8 * half + 8, k * LANES : (k + 1) * LANES
            ]
    row = iota((8, LANES), 0)
    lane = iota((8, LANES), 1) % LX
    inside = (row >= 1) & (row <= kept)
    upper = row < 4
    left = lane < LX // 2
    second = place_ref[2] == 1

    def load(j, k):
        at = chunk * (PARTS * j + k)
        return jnp.where(inside, pltpu.roll(got_ref[at : at + 8, :], 1, 0), 0.0)

    for k in range(PARTS):
        column = [load(j, k) for j in range(PARTS)]
        for j in range(PARTS):
            beside = jnp.where(upper, column[(j + 1) % PARTS], column[(j - 1) % PARTS])
            at = 8 * (PARTS * j + k)
            work[at : at + 8, :] = column[j] + pltpu.roll(beside, 4, 0)
    for j in range(PARTS):
        line = [work[8 * (PARTS * j + k) : 8 * (PARTS * j + k) + 8, :] for k in range(PARTS)]
        for k in range(PARTS):
            beside = jnp.where(left, line[(k + 1) % PARTS], line[(k - 1) % PARTS])
            half = LX // 2
            value = line[k] + jnp.where(
                left, pltpu.roll(beside, LANES - half, 1), pltpu.roll(beside, half, 1)
            )
            value = jnp.where(second, pltpu.roll(value, 4, 0), value)
            at = out_chunk * (PARTS * j + k) + 2
            send_ref[at : at + 4, :] = value[0:4]


def on_plane(place, lx, got):
    t = TABLES
    return call(
        plane_kernel,
        jax.ShapeDtypeStruct((64 * 6, LANES), F32),
        [SMEM, SMEM] + [VMEM] * 10,
        [pltpu.VMEM((64 * 8, LANES), F32)],
        name="on_plane",
    )(
        place,
        lx,
        got,
        *map(jnp.asarray, t["z_table"]),
        *map(jnp.asarray, t["y_table"]),
        jnp.asarray(t["wave_yz"]),
        *map(jnp.asarray, t["y_back"]),
        *map(jnp.asarray, t["z_back"]),
    )


def cube_root(value):
    safe = jnp.maximum(value, 1e-30)
    root = jnp.exp(jnp.log(safe) * (1.0 / 3.0))
    root = root - (root - safe / (root * root)) * (1.0 / 3.0)
    return jnp.where(value > 0.0, root, 0.0)


def exchange_correlation(density):
    root = cube_root(density)
    slater = -((3.0 / math.pi) ** (1.0 / 3.0)) * root
    radius = (3.0 / (4.0 * math.pi)) ** (1.0 / 3.0)
    bottom = radius + 7.8 * root
    wigner = -0.44 * root / bottom * (1.0 + radius / (3.0 * bottom))
    return slater + wigner


def window_kernel(got_ref, ion_ref, send_ref, dens_ref, base_ref):
    for half in range(2):
        value = got_ref[pl.ds(half, 64, stride=6), :]
        for s in range(PARTS):
            send_ref[pl.ds(s * LANES + half, 64, stride=2), :] = value
    for q in range(2):
        for y in range(4):
            here = slice((4 * q + y) * LANES, (4 * q + y + 1) * LANES)
            value = got_ref[pl.ds(6 * q + 2 + y, LX, stride=12), :]
            dens_ref[:, here] = value
            base_ref[:, here] = ion_ref[:, here] + exchange_correlation(value)


def on_window(got, ion_ext):
    return call(
        window_kernel,
        (
            jax.ShapeDtypeStruct((PARTS * LANES, LANES), F32),
            jax.ShapeDtypeStruct((LX, LX * LX), F32),
            jax.ShapeDtypeStruct((LX, LX * LX), F32),
        ),
        [VMEM, VMEM],
        name="on_window",
    )(got, ion_ext)


def last_kernel(place_ref, got_ref, base_ref, high_ref, low_ref, out_ref):
    at = place_ref[0]
    table = (high_ref[at], low_ref[at])
    for y in range(8):
        here = slice(y * LANES, (y + 1) * LANES)
        lines = got_ref[pl.ds(y, N, stride=8), :]
        out_ref[:, here] = base_ref[:, here] + dot3(table, halves(lines))


def last_step(place, got, base):
    return call(
        last_kernel,
        jax.ShapeDtypeStruct((LX, LX * LX), F32),
        [SMEM, VMEM, VMEM, VMEM, VMEM],
        name="last_step",
    )(place, got, base, *map(jnp.asarray, TABLES["last"]))


def both_sides(first, last, axis):
    count = lax.axis_size(axis)
    up = [(i, (i + 1) % count) for i in range(count)]
    down = [(j, i) for i, j in up]
    return lax.ppermute(last, axis, up), lax.ppermute(first, axis, down)


def refill(fields):
    both = jnp.stack(fields)
    count = both.shape[0] * CORE
    slab = (count, CORE * BUF)
    before, after = both_sides(
        both[..., :BUF].reshape(slab), both[..., CORE - BUF :].reshape(slab), "gz"
    )
    shape = (len(fields), CORE, CORE, BUF)
    both = jnp.concatenate([before.reshape(shape), both, after.reshape(shape)], axis=3)
    both = both.reshape(count, CORE * LX)
    width = BUF * LX
    before, after = both_sides(both[:, :width], both[:, CORE * LX - width :], "gy")
    both = jnp.concatenate([before, both, after], axis=1).reshape(len(fields), CORE, LX * LX)
    before, after = both_sides(both[:, :BUF], both[:, CORE - BUF :], "gx")
    return jnp.concatenate([before, both, after], axis=1)


def exchange(value, axis, rows):
    parts = value.shape[0] // rows
    tile = math.gcd(rows, 8)
    shaped = value.reshape(value.shape[0] // tile, tile, LANES)
    return lax.all_to_all(shaped, axis, split_axis=0, concat_axis=0, tiled=True).reshape(
        value.shape
    )


def on_device(orbitals, potential, ion_potential, occupations):
    gx, member = lax.axis_index("gx"), lax.axis_index(("gy", "gz"))
    place = jnp.stack([gx, member % 4, member % 2]).astype(jnp.int32)
    lx = jnp.asarray(TABLES["wave"])[gx * CORE + member // 4].reshape(1)
    window = refill((potential, ion_potential))
    new_orbitals, send = filtered_set(occupations, orbitals, window[0])
    got = exchange(send, "gx", KEPT * KEPT // PER)
    send = along_x(place, got)
    got = exchange(send, ("gy", "gz"), 2 * KEPT // PER)
    send = on_plane(place, lx, got)
    got = exchange(send, ("gy", "gz"), 6)
    send, dens, base = on_window(got, window[1])
    density = dens[BUF : BUF + CORE].reshape(CORE, LX, LX)[
        :, BUF : BUF + CORE, BUF : BUF + CORE
    ]
    got = exchange(send, "gx", LANES)
    new_potential = last_step(place, got, base)
    return (new_orbitals, density, new_potential)


def solution(mesh):
    placed = (P(None, "gx", ("gy", "gz")), P("gx", "gy", "gz"), P("gx", "gy", "gz"), P())
    return jax.shard_map(
        on_device,
        mesh=mesh,
        in_specs=placed,
        out_specs=(P(None, "gx", ("gy", "gz")), P("gx", "gy", "gz"), P("gx", ("gy", "gz"))),
        check_vma=False,
    )
```

```python
import functools
import math

import jax
import jax.numpy as jnp
import numpy as np
from jax import lax
from jax.experimental import pallas as pl
from jax.experimental.pallas import tpu as pltpu
from jax.sharding import PartitionSpec as P

BUF = 8
DEGREE = 10
N = 128
CORE = 16
LX = 32
NORB = 8
PARTS = 8
FIRST, LAST = 4, 28
KEPT = LAST - FIRST
LANES = 128
GROUP = 16
PER = LANES // LX

spacing = 0.2
kinetic = 0.5 / (spacing * spacing)
filter_low = 6.0
filter_high = 12.0 * kinetic
centre_value = 0.5 * (filter_low + filter_high)
half_width = 0.5 * (filter_high - filter_low)

F32, BF16 = jnp.float32, jnp.bfloat16
VMEM = pl.BlockSpec(memory_space=pltpu.VMEM)
SMEM = pl.BlockSpec(memory_space=pltpu.SMEM)
INTERPRET = False


def call(kernel, out_shape, in_specs, scratch=(), flops=1000000, name=None):
    many = isinstance(out_shape, (tuple, list))
    return pl.pallas_call(
        kernel,
        out_shape=out_shape,
        in_specs=in_specs,
        out_specs=tuple(VMEM for _ in out_shape) if many else VMEM,
        scratch_shapes=scratch,
        compiler_params=pltpu.CompilerParams(vmem_limit_bytes=40 * 1024 * 1024),
        cost_estimate=pl.CostEstimate(flops=flops, bytes_accessed=1000000, transcendentals=0),
        interpret=INTERPRET,
        name=name,
    )


def _basis():
    n = np.arange(N, dtype=np.float64)
    angle = 2.0 * np.pi * np.mod(np.outer(n, n), N) / N
    return (np.cos(angle) + np.sin(angle)) / math.sqrt(N)


def _pair(table):
    high = np.asarray(table, np.float32).astype(jnp.bfloat16)
    low = (np.asarray(table, np.float64) - high.astype(np.float64)).astype(jnp.bfloat16)
    return high, low


def _cell(part, a):
    return np.mod(CORE * part + a - BUF, N)


def _tables():
    basis = _basis()
    parts = np.arange(PARTS)
    along = np.zeros((PARTS, CORE + LX, PARTS * KEPT))
    for i in range(PARTS):
        for other in range(PARTS):
            for xx in range(KEPT):
                column = other * KEPT + xx
                cell = _cell(other, xx + FIRST)
                along[i, :CORE, column] = basis[CORE * i : CORE * (i + 1), cell]
                for a in range(LX):
                    if _cell(i, a) == cell and min((other - i) % PARTS, (i - other) % PARTS) <= 1:
                        along[i, CORE + a, column] = 1.0
    lane = np.arange(PARTS * LANES)
    z_cell = _cell(lane // LANES, lane % LX)
    z_table = basis[z_cell, :]
    y_lo, y_hi, j = np.meshgrid(np.arange(PER), np.arange(KEPT // PER), parts, indexing="ij")
    y_table = basis[:, _cell(j, FIRST + PER * y_hi + y_lo).reshape(-1)]
    back = np.zeros((4, 64, N))
    for q in range(4):
        y_lo, y_half, j = np.meshgrid(np.arange(PER), np.arange(2), parts, indexing="ij")
        back[q] = basis[_cell(j, 8 * q + PER * y_half + y_lo).reshape(-1), :]
    last = np.stack([basis[_cell(i, np.arange(LX)), :] for i in range(PARTS)])
    wave = 4.0 / (spacing * spacing) * np.sin(np.pi * np.arange(N) / N) ** 2
    return dict(
        along=_pair(along),
        z_table=_pair(z_table),
        z_back=_pair(z_table.T),
        y_table=_pair(y_table),
        y_back=_pair(back),
        last=_pair(last),
        wave=wave.astype(np.float32),
        wave_yz=(wave[:, None] + wave[None, :]).astype(np.float32),
    )


def _weight():
    position = np.arange(LX, dtype=np.float32)
    rising = np.clip((position + 0.5 - 0.5 * BUF) / BUF, 0.0, 1.0)
    falling = np.clip((LX - 0.5 * BUF - 0.5 - position) / BUF, 0.0, 1.0)
    profile = (rising * falling).astype(np.float32)
    return profile[:, None] * (profile[:, None] * profile[None, :]).reshape(1, LX * LX)


TABLES = _tables()
WEIGHT = _weight().astype(np.float32)


def halves(value):
    high = value.astype(BF16)
    return high, (value - high.astype(F32)).astype(BF16)


def dot3(left, right):
    def one(a, b):
        return jnp.dot(a, b, preferred_element_type=F32)

    return one(left[0], right[0]) + (one(left[0], right[1]) + one(left[1], right[0]))


def iota(shape, dim):
    return lax.broadcasted_iota(jnp.int32, shape, dim)


def swap_four(v, lane):
    low, even = lane < 2 * LX, (lane // LX) % 2 == 0
    w = [None] * 4
    for g in range(2):
        w[g] = jnp.where(low, v[g], pltpu.roll(v[g + 2], 2 * LX, 1))
        w[g + 2] = jnp.where(low, pltpu.roll(v[g], 2 * LX, 1), v[g + 2])
    out = []
    for g in (0, 2):
        out.append(jnp.where(even, w[g], pltpu.roll(w[g + 1], LX, 1)))
        out.append(jnp.where(even, pltpu.roll(w[g], 3 * LX, 1), w[g + 1]))
    return out


def swap_inner(v, row, lane):
    a, b = row % 4, lane // LX
    turned = pltpu.roll(v, 2 * LX, 1)
    v = jnp.where(
        a // 2 == b // 2,
        v,
        jnp.where(a < 2, pltpu.roll(turned, 6, 0), pltpu.roll(turned, 2, 0)),
    )
    return jnp.where(
        a % 2 == b % 2,
        v,
        jnp.where(
            a % 2 == 0,
            pltpu.roll(pltpu.roll(v, LX, 1), 7, 0),
            pltpu.roll(pltpu.roll(v, 3 * LX, 1), 1, 0),
        ),
    )


def filter_kernel(occ_ref, orb_ref, pot_ref, weight_ref, new_ref, send_ref, ya, yb, coef, flat):
    tiles, chunks = LX // 8, LX * LX // LANES
    line = LX + 2
    lane = iota((8, LANES), 1)
    row = iota((8, LANES), 0)
    low_z, high_z = lane % LX == 0, lane % LX == LX - 1
    first_x, last_x = row == 0, row == 7
    zero = jnp.zeros((8, LANES), F32)
    alpha = -2.0 * kinetic / half_width
    scale, shift = 2.0 / half_width, (2.0 / half_width) * (6.0 * kinetic - centre_value)

    for buffer in (ya, yb):
        for h in range(2):
            buffer[h * line] = jnp.zeros((LX, LANES), F32)
            buffer[h * line + line - 1] = jnp.zeros((LX, LANES), F32)

    def bring(c, carry):
        here = pl.ds(pl.multiple_of(c * LANES, LANES), LANES)
        for t in range(tiles):
            rows = slice(8 * t, 8 * t + 8)
            for h in range(2):
                v = [orb_ref[4 * h + g, rows, here].astype(F32) for g in range(4)]
                for y, value in enumerate(swap_four(v, lane)):
                    ya[h * line + 1 + PER * c + y, rows, :] = value
            v = scale * pot_ref[rows, here] + shift
            for y in range(PER):
                value = jnp.where(lane // LX == y, v, 0.0)
                value = value + pltpu.roll(value, LX, 1)
                coef[PER * c + y, rows, :] = value + pltpu.roll(value, 2 * LX, 1)
        return carry

    lax.fori_loop(0, chunks, bring, 0)

    def advance(src, dst, start):
        def one(b, carry):
            for yy in range(GROUP):
                y = GROUP * b + yy
                for h in range(2):
                    at = h * line + 1 + y
                    cells = [src[at, 8 * t : 8 * t + 8, :] for t in range(tiles)]
                    for t in range(tiles):
                        rows = slice(8 * t, 8 * t + 8)
                        cur = cells[t]
                        above = cells[t - 1] if t > 0 else zero
                        below = cells[t + 1] if t < tiles - 1 else zero
                        total = jnp.where(low_z, zero, pltpu.roll(cur, 1, 1))
                        total += jnp.where(high_z, zero, pltpu.roll(cur, LANES - 1, 1))
                        total += pltpu.roll(jnp.where(last_x, above, cur), 1, 0)
                        total += pltpu.roll(jnp.where(first_x, below, cur), 7, 0)
                        total += src[at - 1, rows, :] + src[at + 1, rows, :]
                        result = alpha * total + coef[y, rows, :] * cur
                        if start:
                            dst[at, rows, :] = 0.5 * result
                        else:
                            dst[at, rows, :] = result - dst[at, rows, :]
            return carry

        lax.fori_loop(0, LX // GROUP, one, 0)

    advance(ya, yb, True)

    def two(m, carry):
        advance(yb, ya, False)
        advance(ya, yb, False)
        return carry

    lax.fori_loop(0, (DEGREE - 2) // 2, two, 0)
    advance(yb, ya, False)

    pairs = [(n, m) for n in range(NORB) for m in range(n + 1)]

    def take(c, carry):
        here = pl.ds(pl.multiple_of(c * LANES, LANES), LANES)
        for t in range(tiles):
            rows = slice(8 * t, 8 * t + 8)
            for h in range(2):
                v = [ya[h * line + 1 + PER * c + y, rows, :] for y in range(PER)]
                for g, value in enumerate(swap_four(v, lane)):
                    flat[4 * h + g, rows, here] = value
        return carry

    lax.fori_loop(0, chunks, take, 0)

    def gather(t, sums):
        sums = list(sums)
        rows = pl.ds(pl.multiple_of(8 * t, 8), 8)
        for c in range(chunks):
            f = [flat[n, rows, c * LANES : (c + 1) * LANES] for n in range(NORB)]
            for at, (n, m) in enumerate(pairs):
                sums[at] = sums[at] + f[n] * f[m]
        return tuple(sums)

    sums = lax.fori_loop(0, tiles, gather, tuple(zero for _ in pairs))
    gram = {
        pair: jnp.sum(jnp.sum(s, axis=0, keepdims=True), axis=1, keepdims=True) / float(LX**3)
        for pair, s in zip(pairs, sums)
    }
    factor, inverse, recip = {}, {}, {}
    for j in range(NORB):
        rest = gram[j, j]
        for k in range(j):
            rest = rest - factor[j, k] * factor[j, k]
        recip[j] = 1.0 / jnp.sqrt(rest)
        for n in range(j + 1, NORB):
            value = gram[n, j]
            for k in range(j):
                value = value - factor[n, k] * factor[j, k]
            factor[n, j] = value * recip[j]
    for j in range(NORB):
        inverse[j, j] = recip[j]
        for n in range(j + 1, NORB):
            value = factor[n, j] * inverse[j, j]
            for k in range(j + 1, n):
                value = value + factor[n, k] * inverse[k, j]
            inverse[n, j] = -recip[n] * value
    wide = {pair: jnp.broadcast_to(inverse[pair], (8, LANES)) for pair in pairs}

    kept = KEPT // PER

    def normal(t, carry):
        rows = pl.ds(pl.multiple_of(8 * t, 8), 8)
        for c in range(chunks):
            here = slice(c * LANES, (c + 1) * LANES)
            f = [flat[n, rows, here] for n in range(NORB)]
            total = zero
            for n in range(NORB):
                value = wide[n, 0] * f[0]
                for m in range(1, n + 1):
                    value = value + wide[n, m] * f[m]
                flat[n, rows, here] = value
                total = total + occ_ref[n] * (value * value)
            if 1 <= c <= kept:
                coef[c, rows, :] = swap_inner(total * weight_ref[rows, here], row, lane)
        return carry

    lax.fori_loop(0, tiles, normal, 0)

    def finish(n, carry):
        new_ref[n] = flat[n].astype(BF16)
        return carry

    lax.fori_loop(0, NORB, finish, 0)

    for c in range(kept):
        for x in range(kept):
            value = coef[c + 1, PER * (x + 1) : PER * (x + 2), :]
            for s in range(PARTS):
                start = s * KEPT * kept + PER * c * kept + x
                send_ref[pl.ds(start, PER, stride=kept), :] = value


def filtered_set(occupations, orbitals, potential_ext):
    return call(
        filter_kernel,
        (
            jax.ShapeDtypeStruct((NORB, LX, LX * LX), BF16),
            jax.ShapeDtypeStruct((PARTS * KEPT * KEPT // PER, LANES), F32),
        ),
        [SMEM, VMEM, VMEM, VMEM],
        [
            pltpu.VMEM((2 * (LX + 2), LX, LANES), F32),
            pltpu.VMEM((2 * (LX + 2), LX, LANES), F32),
            pltpu.VMEM((LX, LX, LANES), F32),
            pltpu.VMEM((NORB, LX, LX * LX), F32),
        ],
        flops=60000000,
        name="filter",
    )(occupations, orbitals, potential_ext, jnp.asarray(WEIGHT))


def y_kernel(place_ref, got_ref, high_ref, low_ref, send_ref):
    kept = KEPT // PER
    at = place_ref[0]
    table = (high_ref[at], low_ref[at])
    for c in range(kept):
        lines = got_ref[pl.ds(c, PARTS * KEPT, stride=kept), :]
        value = dot3(table, halves(lines))
        for q in range(2):
            send_ref[pl.ds(q * 2 * kept + c, LX, stride=4 * kept), :] = value[CORE:]
        for q in range(4):
            send_ref[pl.ds(q * 2 * kept + kept + c, CORE, stride=8 * kept), :] = value[:CORE]


def along_y(place, got):
    return call(
        y_kernel,
        jax.ShapeDtypeStruct((64 * 2 * KEPT // PER, LANES), F32),
        [SMEM, VMEM, VMEM, VMEM],
        name="along_y",
    )(place, got, *map(jnp.asarray, TABLES["along"]))


def plane_kernel(
    place_ref,
    own_ref,
    got_ref,
    zh_ref,
    zl_ref,
    yh_ref,
    yl_ref,
    wave_ref,
    bh_ref,
    bl_ref,
    th_ref,
    tl_ref,
    send_ref,
    work,
):
    kept = KEPT // PER
    chunk = 2 * kept
    out_chunk = 6
    wide = PARTS * LANES
    blocks = []
    for k in range(PARTS):
        rows = [
            got_ref[pl.ds(chunk * k + kept + c, PARTS, stride=chunk * PARTS), :]
            for c in range(kept)
        ]
        blocks.append(jnp.concatenate(rows, axis=0))
    lines = jnp.concatenate(blocks, axis=1)
    which = (iota(lines.shape, 1) % LANES) // LX
    spread = jnp.concatenate([jnp.where(which == y, lines, 0.0) for y in range(PER)], axis=0)
    along_z = dot3(halves(spread), (zh_ref[...], zl_ref[...]))
    spectrum = dot3((yh_ref[...], yl_ref[...]), halves(along_z))
    eigen = wave_ref[...] + own_ref[0]
    positive = eigen > 0.0
    green = jnp.where(positive, 4.0 * math.pi / jnp.where(positive, eigen, 1.0), 0.0)
    spectrum = spectrum * green
    quarter = place_ref[1]
    lines = dot3((bh_ref[quarter], bl_ref[quarter]), halves(spectrum))
    spread = dot3(halves(lines), (th_ref[...], tl_ref[...]))
    which = (iota((16, wide), 1) % LANES) // LX
    packed = jnp.zeros((16, wide), F32)
    for y in range(PER):
        packed = jnp.where(which == y, spread[16 * y : 16 * (y + 1)], packed)
    for k in range(PARTS):
        for half in range(2):
            send_ref[pl.ds(out_chunk * k + half, PARTS, stride=out_chunk * PARTS), :] = packed[
                8 * half : 8 * half + 8, k * LANES : (k + 1) * LANES
            ]
    row = iota((8, LANES), 0)
    lane = iota((8, LANES), 1) % LX
    inside = (row >= 1) & (row <= kept)
    upper = row < 4
    left = lane < LX // 2
    second = place_ref[2] == 1

    def load(j, k):
        at = chunk * (PARTS * j + k)
        return jnp.where(inside, pltpu.roll(got_ref[at : at + 8, :], 1, 0), 0.0)

    for k in range(PARTS):
        column = [load(j, k) for j in range(PARTS)]
        for j in range(PARTS):
            beside = jnp.where(upper, column[(j + 1) % PARTS], column[(j - 1) % PARTS])
            at = 8 * (PARTS * j + k)
            work[at : at + 8, :] = column[j] + pltpu.roll(beside, 4, 0)
    for j in range(PARTS):
        line = [work[8 * (PARTS * j + k) : 8 * (PARTS * j + k) + 8, :] for k in range(PARTS)]
        for k in range(PARTS):
            beside = jnp.where(left, line[(k + 1) % PARTS], line[(k - 1) % PARTS])
            half = LX // 2
            value = line[k] + jnp.where(
                left, pltpu.roll(beside, LANES - half, 1), pltpu.roll(beside, half, 1)
            )
            value = jnp.where(second, pltpu.roll(value, 4, 0), value)
            at = out_chunk * (PARTS * j + k) + 2
            send_ref[at : at + 4, :] = value[0:4]


def on_plane(place, wave, got):
    t = TABLES
    return call(
        plane_kernel,
        jax.ShapeDtypeStruct((64 * 6, LANES), F32),
        [SMEM, SMEM] + [VMEM] * 10,
        [pltpu.VMEM((64 * 8, LANES), F32)],
        name="on_plane",
    )(
        place,
        wave,
        got,
        *map(jnp.asarray, t["z_table"]),
        *map(jnp.asarray, t["y_table"]),
        jnp.asarray(t["wave_yz"]),
        *map(jnp.asarray, t["y_back"]),
        *map(jnp.asarray, t["z_back"]),
    )


def cube_root(value):
    safe = jnp.maximum(value, 1e-30)
    root = jnp.exp(jnp.log(safe) * (1.0 / 3.0))
    root = root - (root - safe / (root * root)) * (1.0 / 3.0)
    return jnp.where(value > 0.0, root, 0.0)


def exchange_correlation(density):
    root = cube_root(density)
    slater = -((3.0 / math.pi) ** (1.0 / 3.0)) * root
    radius = (3.0 / (4.0 * math.pi)) ** (1.0 / 3.0)
    bottom = radius + 7.8 * root
    wigner = -0.44 * root / bottom * (1.0 + radius / (3.0 * bottom))
    return slater + wigner


def window_kernel(got_ref, ion_ref, send_ref, dens_ref, base_ref, work):
    for half in range(2):
        value = got_ref[pl.ds(half, 64, stride=6), :]
        for s in range(PARTS):
            send_ref[pl.ds(s * LANES + half, 64, stride=2), :] = value
    row, lane = iota((8, LANES), 0), iota((8, LANES), 1)
    for q in range(2):
        for h in range(4):
            x = 4 * q + h
            value = got_ref[pl.ds(6 * q + 2 + h, LX, stride=12), :]
            if 2 <= x < 6:
                for low in range(PER):
                    core = pltpu.roll(value[BUF : BUF + CORE], LANES - LX * low - BUF, 1)
                    dens_ref[PER * (x - 2) + low] = core[:, :CORE]
            for t in range(4):
                piece = swap_inner(value[8 * t : 8 * t + 8], row, lane)
                for half in range(2):
                    y = 2 * t + half
                    work[PER * x : PER * x + PER, y * LANES : (y + 1) * LANES] = piece[
                        PER * half : PER * half + PER
                    ]
    base_ref[...] = ion_ref[...] + exchange_correlation(work[...])


def on_window(got, ion_ext):
    return call(
        window_kernel,
        (
            jax.ShapeDtypeStruct((PARTS * LANES, LANES), F32),
            jax.ShapeDtypeStruct((CORE, CORE, CORE), F32),
            jax.ShapeDtypeStruct((LX, LX * LX), F32),
        ),
        [VMEM, VMEM],
        [pltpu.VMEM((LX, LX * LX), F32)],
        name="on_window",
    )(got, ion_ext)


def last_kernel(place_ref, got_ref, base_ref, high_ref, low_ref, out_ref):
    at = place_ref[0]
    table = (high_ref[at], low_ref[at])
    row, lane = iota((8, LANES), 0), iota((8, LANES), 1)
    for x in range(8):
        lines = got_ref[pl.ds(x, N, stride=8), :]
        value = dot3(table, halves(lines))
        rows = slice(PER * x, PER * x + PER)
        for t in range(4):
            piece = swap_inner(value[8 * t : 8 * t + 8], row, lane)
            for half in range(2):
                y = 2 * t + half
                here = slice(y * LANES, (y + 1) * LANES)
                out_ref[rows, here] = base_ref[rows, here] + piece[PER * half : PER * half + PER]


def last_step(place, got, base):
    return call(
        last_kernel,
        jax.ShapeDtypeStruct((LX, LX * LX), F32),
        [SMEM, VMEM, VMEM, VMEM, VMEM],
        name="last_step",
    )(place, got, base, *map(jnp.asarray, TABLES["last"]))


def both_sides(first, last, axis):
    count = lax.axis_size(axis)
    up = [(i, (i + 1) % count) for i in range(count)]
    down = [(j, i) for i, j in up]
    return lax.ppermute(last, axis, up), lax.ppermute(first, axis, down)


def refill(fields):
    both = jnp.stack(fields)
    count = both.shape[0] * CORE
    slab = (count, CORE * BUF)
    before, after = both_sides(
        both[..., :BUF].reshape(slab), both[..., CORE - BUF :].reshape(slab), "gz"
    )
    shape = (len(fields), CORE, CORE, BUF)
    both = jnp.concatenate([before.reshape(shape), both, after.reshape(shape)], axis=3)
    both = both.reshape(count, CORE * LX)
    width = BUF * LX
    before, after = both_sides(both[:, :width], both[:, CORE * LX - width :], "gy")
    both = jnp.concatenate([before, both, after], axis=1).reshape(len(fields), CORE, LX * LX)
    before, after = both_sides(both[:, :BUF], both[:, CORE - BUF :], "gx")
    return jnp.concatenate([before, both, after], axis=1)


def exchange(value, axis, rows):
    parts = value.shape[0] // rows
    tile = math.gcd(rows, 8)
    shaped = value.reshape(value.shape[0] // tile, tile, LANES)
    return lax.all_to_all(shaped, axis, split_axis=0, concat_axis=0, tiled=True).reshape(
        value.shape
    )


def on_device(orbitals, potential, ion_potential, occupations):
    gy, member = lax.axis_index("gy"), lax.axis_index(("gx", "gz"))
    place = jnp.stack([gy, member % 4, member % 2]).astype(jnp.int32)
    wave = jnp.asarray(TABLES["wave"])[gy * CORE + member // 4].reshape(1)
    window = refill((potential, ion_potential))
    window, place, wave = lax.optimization_barrier((window, place, wave))
    new_orbitals, send = filtered_set(occupations, orbitals, window[0])
    got = exchange(send, "gy", KEPT * KEPT // PER)
    send = along_y(place, got)
    got = exchange(send, ("gx", "gz"), 2 * KEPT // PER)
    send = on_plane(place, wave, got)
    got = exchange(send, ("gx", "gz"), 6)
    send, density, base = on_window(got, window[1])
    got = exchange(send, "gy", LANES)
    new_potential = last_step(place, got, base)
    return (new_orbitals, density, new_potential)


def solution(mesh):
    placed = (P(None, "gx", ("gy", "gz")), P("gx", "gy", "gz"), P("gx", "gy", "gz"), P())
    return jax.shard_map(
        on_device,
        mesh=mesh,
        in_specs=placed,
        out_specs=(P(None, "gx", ("gy", "gz")), P("gx", "gy", "gz"), P("gx", ("gy", "gz"))),
        check_vma=False,
    )
```

```python
import functools
import math

import jax
import jax.numpy as jnp
import numpy as np
from jax import lax
from jax.experimental import pallas as pl
from jax.experimental.pallas import tpu as pltpu
from jax.sharding import PartitionSpec as P

BUF = 8
DEGREE = 10
N = 128
CORE = 16
LX = 32
NORB = 8
PARTS = 8
FIRST, LAST = 4, 28
KEPT = LAST - FIRST
LANES = 128
CHUNK = 9
GROUP = 16
PER = LANES // LX

spacing = 0.2
kinetic = 0.5 / (spacing * spacing)
filter_low = 6.0
filter_high = 12.0 * kinetic
centre_value = 0.5 * (filter_low + filter_high)
half_width = 0.5 * (filter_high - filter_low)

F32, BF16 = jnp.float32, jnp.bfloat16
VMEM = pl.BlockSpec(memory_space=pltpu.VMEM)
SMEM = pl.BlockSpec(memory_space=pltpu.SMEM)
INTERPRET = False


def call(kernel, out_shape, in_specs, scratch=(), flops=1000000, name=None):
    many = isinstance(out_shape, (tuple, list))
    return pl.pallas_call(
        kernel,
        out_shape=out_shape,
        in_specs=in_specs,
        out_specs=tuple(VMEM for _ in out_shape) if many else VMEM,
        scratch_shapes=scratch,
        compiler_params=pltpu.CompilerParams(vmem_limit_bytes=40 * 1024 * 1024),
        cost_estimate=pl.CostEstimate(flops=flops, bytes_accessed=1000000, transcendentals=0),
        interpret=INTERPRET,
        name=name,
    )


def _basis():
    n = np.arange(N, dtype=np.float64)
    angle = 2.0 * np.pi * np.mod(np.outer(n, n), N) / N
    return (np.cos(angle) + np.sin(angle)) / math.sqrt(N)


def _pair(table):
    high = np.asarray(table, np.float32).astype(jnp.bfloat16)
    low = (np.asarray(table, np.float64) - high.astype(np.float64)).astype(jnp.bfloat16)
    return high, low


def _cell(part, a):
    return np.mod(CORE * part + a - BUF, N)


def _tables():
    basis = _basis()
    parts = np.arange(PARTS)
    along = np.zeros((PARTS, CORE + LX, PARTS * KEPT))
    for i in range(PARTS):
        for other in range(PARTS):
            for xx in range(KEPT):
                column = other * KEPT + xx
                cell = _cell(other, xx + FIRST)
                along[i, :CORE, column] = basis[CORE * i : CORE * (i + 1), cell]
                for a in range(LX):
                    if _cell(i, a) == cell and min((other - i) % PARTS, (i - other) % PARTS) <= 1:
                        along[i, CORE + a, column] = 1.0
    lane = np.arange(PARTS * LANES)
    z_cell = _cell(lane // LANES, lane % LX)
    z_table = basis[z_cell, :]
    y_lo, y_hi, j = np.meshgrid(np.arange(PER), np.arange(KEPT // PER), parts, indexing="ij")
    y_table = basis[:, _cell(j, FIRST + PER * y_hi + y_lo).reshape(-1)]
    back = np.zeros((4, 64, N))
    for q in range(4):
        y_lo, y_half, j = np.meshgrid(np.arange(PER), np.arange(2), parts, indexing="ij")
        back[q] = basis[_cell(j, 8 * q + PER * y_half + y_lo).reshape(-1), :]
    last = np.stack([basis[_cell(i, np.arange(LX)), :] for i in range(PARTS)])
    wave = 4.0 / (spacing * spacing) * np.sin(np.pi * np.arange(N) / N) ** 2
    return dict(
        along=_pair(along),
        z_table=_pair(z_table),
        z_back=_pair(z_table.T),
        y_table=_pair(y_table),
        y_back=_pair(back),
        last=_pair(last),
        wave=wave.astype(np.float32),
        wave_yz=(wave[:, None] + wave[None, :]).astype(np.float32),
    )


def _weight():
    position = np.arange(LX, dtype=np.float32)
    rising = np.clip((position + 0.5 - 0.5 * BUF) / BUF, 0.0, 1.0)
    falling = np.clip((LX - 0.5 * BUF - 0.5 - position) / BUF, 0.0, 1.0)
    profile = (rising * falling).astype(np.float32)
    return profile[:, None] * (profile[:, None] * profile[None, :]).reshape(1, LX * LX)


TABLES = _tables()
WEIGHT = _weight().astype(np.float32)


def halves(value):
    high = value.astype(BF16)
    return high, (value - high.astype(F32)).astype(BF16)


def dot3(left, right):
    def one(a, b):
        return jnp.dot(a, b, preferred_element_type=F32)

    return one(left[0], right[0]) + (one(left[0], right[1]) + one(left[1], right[0]))


def iota(shape, dim):
    return lax.broadcasted_iota(jnp.int32, shape, dim)


def swap_four(v, lane):
    low, even = lane < 2 * LX, (lane // LX) % 2 == 0
    w = [None] * 4
    for g in range(2):
        w[g] = jnp.where(low, v[g], pltpu.roll(v[g + 2], 2 * LX, 1))
        w[g + 2] = jnp.where(low, pltpu.roll(v[g], 2 * LX, 1), v[g + 2])
    out = []
    for g in (0, 2):
        out.append(jnp.where(even, w[g], pltpu.roll(w[g + 1], LX, 1)))
        out.append(jnp.where(even, pltpu.roll(w[g], 3 * LX, 1), w[g + 1]))
    return out


def swap_inner(v, row, lane):
    a, b = row % 4, lane // LX
    turned = pltpu.roll(v, 2 * LX, 1)
    v = jnp.where(
        a // 2 == b // 2,
        v,
        jnp.where(a < 2, pltpu.roll(turned, 6, 0), pltpu.roll(turned, 2, 0)),
    )
    return jnp.where(
        a % 2 == b % 2,
        v,
        jnp.where(
            a % 2 == 0,
            pltpu.roll(pltpu.roll(v, LX, 1), 7, 0),
            pltpu.roll(pltpu.roll(v, 3 * LX, 1), 1, 0),
        ),
    )


def bring_kernel(orb_ref, out_ref):
    tiles, chunks = LX // 8, LX * LX // LANES
    lane = iota((8, LANES), 1)
    line = LX + 2
    for h in range(2):
        out_ref[h * line] = jnp.zeros((LX, LANES), F32)
        out_ref[h * line + line - 1] = jnp.zeros((LX, LANES), F32)

    def bring(c, carry):
        here = pl.ds(pl.multiple_of(c * LANES, LANES), LANES)
        for t in range(tiles):
            rows = slice(8 * t, 8 * t + 8)
            for h in range(2):
                v = [orb_ref[4 * h + g, rows, here].astype(F32) for g in range(4)]
                for y, value in enumerate(swap_four(v, lane)):
                    out_ref[h * line + 1 + PER * c + y, rows, :] = value
        return carry

    lax.fori_loop(0, chunks, bring, 0)


def bring_orbitals(orbitals):
    return call(
        bring_kernel,
        jax.ShapeDtypeStruct((2 * (LX + 2), LX, LANES), F32),
        [VMEM],
        flops=15000000,
        name="bring",
    )(orbitals)


def filter_kernel(occ_ref, orb_ref, pot_ref, weight_ref, new_ref, send_ref, ya, yb, coef, flat):
    tiles, chunks = LX // 8, LX * LX // LANES
    line = LX + 2
    lane = iota((8, LANES), 1)
    row = iota((8, LANES), 0)
    low_z, high_z = lane % LX == 0, lane % LX == LX - 1
    first_x, last_x = row == 0, row == 7
    zero = jnp.zeros((8, LANES), F32)
    alpha = -2.0 * kinetic / half_width
    scale, shift = 2.0 / half_width, (2.0 / half_width) * (6.0 * kinetic - centre_value)

    for buffer in (ya, yb):
        for h in range(2):
            buffer[h * line] = jnp.zeros((LX, LANES), F32)
            buffer[h * line + line - 1] = jnp.zeros((LX, LANES), F32)

    def spread(c, carry):
        here = pl.ds(pl.multiple_of(c * LANES, LANES), LANES)
        for t in range(tiles):
            rows = slice(8 * t, 8 * t + 8)
            v = scale * pot_ref[rows, here] + shift
            for y in range(PER):
                value = jnp.where(lane // LX == y, v, 0.0)
                value = value + pltpu.roll(value, LX, 1)
                coef[PER * c + y, rows, :] = value + pltpu.roll(value, 2 * LX, 1)
        return carry

    lax.fori_loop(0, chunks, spread, 0)

    def advance(src, before, dst):
        def one(b, carry):
            for yy in range(GROUP):
                y = GROUP * b + yy
                for h in range(2):
                    at = h * line + 1 + y
                    cells = [src[at, 8 * t : 8 * t + 8, :] for t in range(tiles)]
                    for t in range(tiles):
                        rows = slice(8 * t, 8 * t + 8)
                        cur = cells[t]
                        above = cells[t - 1] if t > 0 else zero
                        below = cells[t + 1] if t < tiles - 1 else zero
                        total = jnp.where(low_z, zero, pltpu.roll(cur, 1, 1))
                        total += jnp.where(high_z, zero, pltpu.roll(cur, LANES - 1, 1))
                        total += pltpu.roll(jnp.where(last_x, above, cur), 1, 0)
                        total += pltpu.roll(jnp.where(first_x, below, cur), 7, 0)
                        total += src[at - 1, rows, :] + src[at + 1, rows, :]
                        result = alpha * total + coef[y, rows, :] * cur
                        if before is None:
                            dst[at, rows, :] = 0.5 * result
                        else:
                            dst[at, rows, :] = result - before[at, rows, :]
            return carry

        lax.fori_loop(0, LX // GROUP, one, 0)

    advance(orb_ref, None, yb)
    advance(yb, orb_ref, ya)

    def two(m, carry):
        advance(ya, yb, yb)
        advance(yb, ya, ya)
        return carry

    lax.fori_loop(0, (DEGREE - 2) // 2, two, 0)

    pairs = [(n, m) for n in range(NORB) for m in range(n + 1)]

    def take(c, carry):
        here = pl.ds(pl.multiple_of(c * LANES, LANES), LANES)
        for t in range(tiles):
            rows = slice(8 * t, 8 * t + 8)
            for h in range(2):
                v = [ya[h * line + 1 + PER * c + y, rows, :] for y in range(PER)]
                for g, value in enumerate(swap_four(v, lane)):
                    flat[4 * h + g, rows, here] = value
        return carry

    lax.fori_loop(0, chunks, take, 0)

    def gather(t, sums):
        sums = list(sums)
        rows = pl.ds(pl.multiple_of(8 * t, 8), 8)
        for c in range(chunks):
            f = [flat[n, rows, c * LANES : (c + 1) * LANES] for n in range(NORB)]
            for at, (n, m) in enumerate(pairs):
                sums[at] = sums[at] + f[n] * f[m]
        return tuple(sums)

    sums = lax.fori_loop(0, tiles, gather, tuple(zero for _ in pairs))
    gram = {
        pair: jnp.sum(jnp.sum(s, axis=0, keepdims=True), axis=1, keepdims=True) / float(LX**3)
        for pair, s in zip(pairs, sums)
    }
    factor, inverse, recip = {}, {}, {}
    for j in range(NORB):
        rest = gram[j, j]
        for k in range(j):
            rest = rest - factor[j, k] * factor[j, k]
        recip[j] = 1.0 / jnp.sqrt(rest)
        for n in range(j + 1, NORB):
            value = gram[n, j]
            for k in range(j):
                value = value - factor[n, k] * factor[j, k]
            factor[n, j] = value * recip[j]
    for j in range(NORB):
        inverse[j, j] = recip[j]
        for n in range(j + 1, NORB):
            value = factor[n, j] * inverse[j, j]
            for k in range(j + 1, n):
                value = value + factor[n, k] * inverse[k, j]
            inverse[n, j] = -recip[n] * value
    wide = {pair: jnp.broadcast_to(inverse[pair], (8, LANES)) for pair in pairs}

    kept = KEPT // PER

    def normal(t, carry):
        rows = pl.ds(pl.multiple_of(8 * t, 8), 8)
        for c in range(chunks):
            here = slice(c * LANES, (c + 1) * LANES)
            f = [flat[n, rows, here] for n in range(NORB)]
            total = zero
            for n in range(NORB):
                value = wide[n, 0] * f[0]
                for m in range(1, n + 1):
                    value = value + wide[n, m] * f[m]
                flat[n, rows, here] = value
                total = total + occ_ref[n] * (value * value)
            if 1 <= c <= kept:
                coef[c, rows, :] = swap_inner(total * weight_ref[rows, here], row, lane)
        return carry

    lax.fori_loop(0, tiles, normal, 0)

    def finish(n, carry):
        new_ref[n] = flat[n].astype(BF16)
        return carry

    lax.fori_loop(0, NORB, finish, 0)

    for c in range(kept):
        for x in range(kept):
            value = coef[c + 1, PER * (x + 1) : PER * (x + 2), :]
            for s in range(PARTS):
                start = s * KEPT * kept + PER * c * kept + x
                send_ref[pl.ds(start, PER, stride=kept), :] = value


def filtered_set(occupations, orbitals, potential_ext):
    return call(
        filter_kernel,
        (
            jax.ShapeDtypeStruct((NORB, LX, LX * LX), BF16),
            jax.ShapeDtypeStruct((PARTS * KEPT * KEPT // PER, LANES), F32),
        ),
        [SMEM, VMEM, VMEM, VMEM],
        [
            pltpu.VMEM((2 * (LX + 2), LX, LANES), F32),
            pltpu.VMEM((2 * (LX + 2), LX, LANES), F32),
            pltpu.VMEM((LX, LX, LANES), F32),
            pltpu.VMEM((NORB, LX, LX * LX), F32),
        ],
        flops=60000000,
        name="filter",
    )(occupations, orbitals, potential_ext, jnp.asarray(WEIGHT))


def y_kernel(place_ref, got_ref, high_ref, low_ref, send_ref):
    kept = KEPT // PER
    part = kept // 2
    chunk = kept + part
    at = place_ref[0]
    odd = place_ref[3] == 1
    table = (high_ref[at], low_ref[at])
    folded = []
    for c in range(kept):
        lines = got_ref[pl.ds(c, PARTS * KEPT, stride=kept), :]
        value = dot3(table, halves(lines))
        folded.append(value[CORE:])
        for q in range(4):
            send_ref[pl.ds(q * chunk + part + c, CORE, stride=4 * chunk), :] = value[:CORE]
    for c in range(part):
        low, high = folded[c], folded[part + c]
        send_ref[pl.ds(c, LX, stride=2 * chunk), :] = jnp.where(odd, high, low)
        send_ref[pl.ds(chunk + c, LX, stride=2 * chunk), :] = jnp.where(odd, low, high)


def along_y(place, got):
    return call(
        y_kernel,
        jax.ShapeDtypeStruct((64 * CHUNK, LANES), F32),
        [SMEM, VMEM, VMEM, VMEM],
        name="along_y",
    )(place, got, *map(jnp.asarray, TABLES["along"]))


def plane_kernel(
    place_ref,
    own_ref,
    got_ref,
    zh_ref,
    zl_ref,
    yh_ref,
    yl_ref,
    wave_ref,
    bh_ref,
    bl_ref,
    th_ref,
    tl_ref,
    send_ref,
    work,
):
    kept = KEPT // PER
    part = kept // 2
    chunk = kept + part
    out_chunk = 6
    wide = PARTS * LANES
    blocks = []
    for k in range(PARTS):
        rows = [
            got_ref[pl.ds(chunk * k + part + c, PARTS, stride=chunk * PARTS), :]
            for c in range(kept)
        ]
        blocks.append(jnp.concatenate(rows, axis=0))
    lines = jnp.concatenate(blocks, axis=1)
    which = (iota(lines.shape, 1) % LANES) // LX
    spread = jnp.concatenate([jnp.where(which == y, lines, 0.0) for y in range(PER)], axis=0)
    along_z = dot3(halves(spread), (zh_ref[...], zl_ref[...]))
    spectrum = dot3((yh_ref[...], yl_ref[...]), halves(along_z))
    eigen = wave_ref[...] + own_ref[0]
    positive = eigen > 0.0
    green = jnp.where(positive, 4.0 * math.pi / jnp.where(positive, eigen, 1.0), 0.0)
    spectrum = spectrum * green
    quarter = place_ref[1]
    lines = dot3((bh_ref[quarter], bl_ref[quarter]), halves(spectrum))
    spread = dot3(halves(lines), (th_ref[...], tl_ref[...]))
    which = (iota((16, wide), 1) % LANES) // LX
    packed = jnp.zeros((16, wide), F32)
    for y in range(PER):
        packed = jnp.where(which == y, spread[16 * y : 16 * (y + 1)], packed)
    for k in range(PARTS):
        for half in range(2):
            send_ref[pl.ds(out_chunk * k + half, PARTS, stride=out_chunk * PARTS), :] = packed[
                8 * half : 8 * half + 8, k * LANES : (k + 1) * LANES
            ]
    row = iota((8, LANES), 0)
    left = iota((8, LANES), 1) % LX < LX // 2
    half = LX // 2
    first, second = row < part, place_ref[2] == 1

    def load(i, k):
        at = chunk * (PARTS * i + k)
        return jnp.where(first, got_ref[at : at + 8, :], 0.0)

    for k in range(PARTS):
        column = [load(i, k) for i in range(PARTS)]
        for m in range(PARTS):
            at = 8 * (PARTS * m + k)
            work[at : at + 8, :] = pltpu.roll(column[m], 1, 0) + column[m - 1]
    for m in range(PARTS):
        after = (m + 1) % PARTS
        other = second if m % 2 == 0 else jnp.logical_not(second)
        line = []
        for k in range(PARTS):
            here, there = 8 * (PARTS * m + k), 8 * (PARTS * after + k)
            line.append(jnp.where(other, work[there : there + 8, :], work[here : here + 8, :]))
        for k in range(PARTS):
            beside = jnp.where(left, line[(k + 1) % PARTS], line[(k - 1) % PARTS])
            value = line[k] + jnp.where(
                left, pltpu.roll(beside, LANES - half, 1), pltpu.roll(beside, half, 1)
            )
            at = out_chunk * (PARTS * m + k) + 2
            send_ref[at : at + 4, :] = value[0:4]


def on_plane(place, wave, got):
    t = TABLES
    return call(
        plane_kernel,
        jax.ShapeDtypeStruct((64 * 6, LANES), F32),
        [SMEM, SMEM] + [VMEM] * 10,
        [pltpu.VMEM((64 * 8, LANES), F32)],
        name="on_plane",
    )(
        place,
        wave,
        got,
        *map(jnp.asarray, t["z_table"]),
        *map(jnp.asarray, t["y_table"]),
        jnp.asarray(t["wave_yz"]),
        *map(jnp.asarray, t["y_back"]),
        *map(jnp.asarray, t["z_back"]),
    )


def cube_root(value):
    safe = jnp.maximum(value, 1e-30)
    root = jnp.exp(jnp.log(safe) * (1.0 / 3.0))
    root = root - (root - safe / (root * root)) * (1.0 / 3.0)
    return jnp.where(value > 0.0, root, 0.0)


def exchange_correlation(density):
    root = cube_root(density)
    slater = -((3.0 / math.pi) ** (1.0 / 3.0)) * root
    radius = (3.0 / (4.0 * math.pi)) ** (1.0 / 3.0)
    bottom = radius + 7.8 * root
    wigner = -0.44 * root / bottom * (1.0 + radius / (3.0 * bottom))
    return slater + wigner


def window_kernel(place_ref, got_ref, ion_ref, send_ref, dens_ref, base_ref, work):
    for half in range(2):
        value = got_ref[pl.ds(half, 64, stride=6), :]
        for s in range(PARTS):
            send_ref[pl.ds(s * LANES + half, 64, stride=2), :] = value
    row, lane = iota((8, LANES), 0), iota((8, LANES), 1)
    odd = place_ref[3] == 1
    for q in range(2):
        for h in range(4):
            x = 4 * q + h
            value = jnp.where(
                odd,
                got_ref[pl.ds(6 * (1 - q) + 2 + h, LX, stride=12), :],
                got_ref[pl.ds(6 * q + 2 + h, LX, stride=12), :],
            )
            if 2 <= x < 6:
                for low in range(PER):
                    core = pltpu.roll(value[BUF : BUF + CORE], LANES - LX * low - BUF, 1)
                    dens_ref[PER * (x - 2) + low] = core[:, :CORE]
            for t in range(4):
                piece = swap_inner(value[8 * t : 8 * t + 8], row, lane)
                for half in range(2):
                    y = 2 * t + half
                    work[PER * x : PER * x + PER, y * LANES : (y + 1) * LANES] = piece[
                        PER * half : PER * half + PER
                    ]
    base_ref[...] = ion_ref[...] + exchange_correlation(work[...])


def on_window(place, got, ion_ext):
    return call(
        window_kernel,
        (
            jax.ShapeDtypeStruct((PARTS * LANES, LANES), F32),
            jax.ShapeDtypeStruct((CORE, CORE, CORE), F32),
            jax.ShapeDtypeStruct((LX, LX * LX), F32),
        ),
        [SMEM, VMEM, VMEM],
        [pltpu.VMEM((LX, LX * LX), F32)],
        name="on_window",
    )(place, got, ion_ext)


def last_kernel(place_ref, got_ref, base_ref, high_ref, low_ref, out_ref):
    at = place_ref[0]
    table = (high_ref[at], low_ref[at])
    row, lane = iota((8, LANES), 0), iota((8, LANES), 1)
    for x in range(8):
        lines = got_ref[pl.ds(x, N, stride=8), :]
        value = dot3(table, halves(lines))
        rows = slice(PER * x, PER * x + PER)
        for t in range(4):
            piece = swap_inner(value[8 * t : 8 * t + 8], row, lane)
            for half in range(2):
                y = 2 * t + half
                here = slice(y * LANES, (y + 1) * LANES)
                out_ref[rows, here] = base_ref[rows, here] + piece[PER * half : PER * half + PER]


def last_step(place, got, base):
    return call(
        last_kernel,
        jax.ShapeDtypeStruct((LX, LX * LX), F32),
        [SMEM, VMEM, VMEM, VMEM, VMEM],
        name="last_step",
    )(place, got, base, *map(jnp.asarray, TABLES["last"]))


def both_sides(first, last, axis):
    count = lax.axis_size(axis)
    up = [(i, (i + 1) % count) for i in range(count)]
    down = [(j, i) for i, j in up]
    return lax.ppermute(last, axis, up), lax.ppermute(first, axis, down)


def pack_kernel(pot_ref, ion_ref, own_ref, up_ref, down_ref):
    lane = iota((CORE, LANES), 1)
    third = (lane % LX) // BUF
    for f, ref in enumerate((pot_ref, ion_ref)):
        rows = slice(CORE * f, CORE * (f + 1))
        up, down = jnp.zeros((CORE, LANES), F32), jnp.zeros((CORE, LANES), F32)
        for c in range(PER):
            value = jnp.zeros((CORE, LANES), F32)
            for y in range(PER):
                line = ref[pl.ds(PER * c + y, CORE, stride=CORE), :]
                line = jnp.concatenate([line, jnp.zeros((CORE, LANES - CORE), F32)], axis=1)
                value = value + pltpu.roll(line, LX * y + BUF, 1)
            own_ref[rows, c * LANES : (c + 1) * LANES] = value
            up = jnp.where(third == c, pltpu.roll(value, (BUF * c - 2 * BUF) % LANES, 1), up)
            down = jnp.where(third == c, pltpu.roll(value, (BUF * c - BUF) % LANES, 1), down)
        up_ref[rows, :] = up
        down_ref[rows, :] = down


def merge_kernel(own_ref, before_ref, after_ref, out_ref):
    third = (iota((2 * CORE, LANES), 1) % LX) // BUF
    before, after = before_ref[...], after_ref[...]
    for c in range(PER):
        here = slice(c * LANES, (c + 1) * LANES)
        value = jnp.where(third == 0, pltpu.roll(before, (-BUF * c) % LANES, 1), own_ref[:, here])
        out_ref[:, here] = jnp.where(
            third == 3, pltpu.roll(after, (3 * BUF - BUF * c) % LANES, 1), value
        )


def refill(fields):
    count = len(fields) * CORE
    slab = jax.ShapeDtypeStruct((count, LANES), F32)
    full = jax.ShapeDtypeStruct((count, CORE * LX), F32)
    own, up, down = call(pack_kernel, (full, slab, slab), [VMEM, VMEM], name="pack")(
        *[f.reshape(CORE * CORE, CORE) for f in fields]
    )
    before, after = both_sides(down, up, "gz")
    both = call(merge_kernel, full, [VMEM, VMEM, VMEM], name="merge")(own, before, after)
    width = BUF * LX
    before, after = both_sides(both[:, :width], both[:, CORE * LX - width :], "gy")
    both = jnp.concatenate([before, both, after], axis=1).reshape(len(fields), CORE, LX * LX)
    before, after = both_sides(both[:, :BUF], both[:, CORE - BUF :], "gx")
    return jnp.concatenate([before, both, after], axis=1)


def exchange(value, axis, rows):
    parts = value.shape[0] // rows
    tile = math.gcd(rows, 8)
    shaped = value.reshape(value.shape[0] // tile, tile, LANES)
    return lax.all_to_all(shaped, axis, split_axis=0, concat_axis=0, tiled=True).reshape(
        value.shape
    )


def on_device(orbitals, potential, ion_potential, occupations):
    gy, member = lax.axis_index("gy"), lax.axis_index(("gx", "gz"))
    place = jnp.stack([gy, member % 4, member % 2, lax.axis_index("gx") % 2]).astype(jnp.int32)
    wave = jnp.asarray(TABLES["wave"])[gy * CORE + member // 4].reshape(1)
    orbitals = bring_orbitals(orbitals)
    window = refill((potential, ion_potential))
    window, place, wave = lax.optimization_barrier((window, place, wave))
    new_orbitals, send = filtered_set(occupations, orbitals, window[0])
    got = exchange(send, "gy", KEPT * KEPT // PER)
    send = along_y(place, got)
    got = exchange(send, ("gx", "gz"), CHUNK)
    send = on_plane(place, wave, got)
    got = exchange(send, ("gx", "gz"), 6)
    send, density, base = on_window(place, got, window[1])
    got = exchange(send, "gy", LANES)
    new_potential = last_step(place, got, base)
    return (new_orbitals, density, new_potential)


def solution(mesh):
    placed = (P(None, "gx", ("gy", "gz")), P("gx", "gy", "gz"), P("gx", "gy", "gz"), P())
    return jax.shard_map(
        on_device,
        mesh=mesh,
        in_specs=placed,
        out_specs=(P(None, "gx", ("gy", "gz")), P("gx", "gy", "gz"), P("gx", ("gy", "gz"))),
        check_vma=False,
    )
```

```python
import functools
import math

import jax
import jax.numpy as jnp
import numpy as np
from jax import lax
from jax.experimental import pallas as pl
from jax.experimental.pallas import tpu as pltpu
from jax.sharding import PartitionSpec as P

BUF = 8
DEGREE = 10
N = 128
CORE = 16
LX = 32
NORB = 8
PARTS = 8
FIRST, LAST = 4, 28
KEPT = LAST - FIRST
LANES = 128
CHUNK = 9
GROUP = 16
PER = LANES // LX

spacing = 0.2
kinetic = 0.5 / (spacing * spacing)
filter_low = 6.0
filter_high = 12.0 * kinetic
centre_value = 0.5 * (filter_low + filter_high)
half_width = 0.5 * (filter_high - filter_low)

F32, BF16 = jnp.float32, jnp.bfloat16
VMEM = pl.BlockSpec(memory_space=pltpu.VMEM)
HBM = pl.BlockSpec(memory_space=pltpu.HBM)
INTERPRET = False


def call(kernel, out_shape, in_specs, scratch=(), flops=1000000, name=None):
    many = isinstance(out_shape, (tuple, list))
    return pl.pallas_call(
        kernel,
        out_shape=out_shape,
        in_specs=in_specs,
        out_specs=tuple(VMEM for _ in out_shape) if many else VMEM,
        scratch_shapes=scratch,
        compiler_params=pltpu.CompilerParams(vmem_limit_bytes=40 * 1024 * 1024),
        cost_estimate=pl.CostEstimate(flops=flops, bytes_accessed=1000000, transcendentals=0),
        interpret=INTERPRET,
        name=name,
    )


def _basis():
    n = np.arange(N, dtype=np.float64)
    angle = 2.0 * np.pi * np.mod(np.outer(n, n), N) / N
    return (np.cos(angle) + np.sin(angle)) / math.sqrt(N)


def _pair(table):
    high = np.asarray(table, np.float32).astype(jnp.bfloat16)
    low = (np.asarray(table, np.float64) - high.astype(np.float64)).astype(jnp.bfloat16)
    return high, low


def _cell(part, a):
    return np.mod(CORE * part + a - BUF, N)


def _tables():
    basis = _basis()
    parts = np.arange(PARTS)
    along = np.zeros((PARTS, CORE + LX, PARTS * KEPT))
    for i in range(PARTS):
        for other in range(PARTS):
            for xx in range(KEPT):
                column = other * KEPT + xx
                cell = _cell(other, xx + FIRST)
                along[i, :CORE, column] = basis[CORE * i : CORE * (i + 1), cell]
                for a in range(LX):
                    if _cell(i, a) == cell and min((other - i) % PARTS, (i - other) % PARTS) <= 1:
                        along[i, CORE + a, column] = 1.0
    lane = np.arange(PARTS * LANES)
    z_cell = _cell(lane // LANES, lane % LX)
    z_table = basis[z_cell, :]
    y_lo, y_hi, j = np.meshgrid(np.arange(PER), np.arange(KEPT // PER), parts, indexing="ij")
    y_table = basis[:, _cell(j, FIRST + PER * y_hi + y_lo).reshape(-1)]
    back = np.zeros((4, 64, N))
    for q in range(4):
        y_lo, y_half, j = np.meshgrid(np.arange(PER), np.arange(2), parts, indexing="ij")
        back[q] = basis[_cell(j, 8 * q + PER * y_half + y_lo).reshape(-1), :]
    last = np.stack([basis[_cell(i, np.arange(LX)), :] for i in range(PARTS)])
    wave = 4.0 / (spacing * spacing) * np.sin(np.pi * np.arange(N) / N) ** 2
    return dict(
        along=_pair(along),
        z_table=_pair(z_table),
        z_back=_pair(z_table.T),
        y_table=_pair(y_table),
        y_back=_pair(back),
        last=_pair(last),
        wave=np.repeat(wave.astype(np.float32)[:, None], LANES, axis=1),
        wave_yz=(wave[:, None] + wave[None, :]).astype(np.float32),
    )


def _weight():
    position = np.arange(LX, dtype=np.float32)
    rising = np.clip((position + 0.5 - 0.5 * BUF) / BUF, 0.0, 1.0)
    falling = np.clip((LX - 0.5 * BUF - 0.5 - position) / BUF, 0.0, 1.0)
    profile = (rising * falling).astype(np.float32)
    return profile[:, None] * (profile[:, None] * profile[None, :]).reshape(1, LX * LX)


TABLES = _tables()
WEIGHT = _weight().astype(np.float32)


def halves(value):
    high = value.astype(BF16)
    return high, (value - high.astype(F32)).astype(BF16)


def dot3(left, right):
    def one(a, b):
        return jnp.dot(a, b, preferred_element_type=F32)

    return one(left[0], right[0]) + (one(left[0], right[1]) + one(left[1], right[0]))


def iota(shape, dim):
    return lax.broadcasted_iota(jnp.int32, shape, dim)


def swap_four(v, lane):
    low, even = lane < 2 * LX, (lane // LX) % 2 == 0
    w = [None] * 4
    for g in range(2):
        w[g] = jnp.where(low, v[g], pltpu.roll(v[g + 2], 2 * LX, 1))
        w[g + 2] = jnp.where(low, pltpu.roll(v[g], 2 * LX, 1), v[g + 2])
    out = []
    for g in (0, 2):
        out.append(jnp.where(even, w[g], pltpu.roll(w[g + 1], LX, 1)))
        out.append(jnp.where(even, pltpu.roll(w[g], 3 * LX, 1), w[g + 1]))
    return out


def swap_inner(v, row, lane):
    a, b = row % 4, lane // LX
    turned = pltpu.roll(v, 2 * LX, 1)
    v = jnp.where(
        a // 2 == b // 2,
        v,
        jnp.where(a < 2, pltpu.roll(turned, 6, 0), pltpu.roll(turned, 2, 0)),
    )
    return jnp.where(
        a % 2 == b % 2,
        v,
        jnp.where(
            a % 2 == 0,
            pltpu.roll(pltpu.roll(v, LX, 1), 7, 0),
            pltpu.roll(pltpu.roll(v, 3 * LX, 1), 1, 0),
        ),
    )


def bring_kernel(orb_ref, out_ref):
    tiles, chunks = LX // 8, LX * LX // LANES
    lane = iota((8, LANES), 1)
    line = LX + 2
    for h in range(2):
        out_ref[h * line] = jnp.zeros((LX, LANES), F32)
        out_ref[h * line + line - 1] = jnp.zeros((LX, LANES), F32)

    def bring(c, carry):
        here = pl.ds(pl.multiple_of(c * LANES, LANES), LANES)
        for t in range(tiles):
            rows = slice(8 * t, 8 * t + 8)
            for h in range(2):
                v = [orb_ref[4 * h + g, rows, here].astype(F32) for g in range(4)]
                for y, value in enumerate(swap_four(v, lane)):
                    out_ref[h * line + 1 + PER * c + y, rows, :] = value
        return carry

    lax.fori_loop(0, chunks, bring, 0)


def bring_orbitals(orbitals):
    return call(
        bring_kernel,
        jax.ShapeDtypeStruct((2 * (LX + 2), LX, LANES), F32),
        [VMEM],
        flops=15000000,
        name="bring",
    )(orbitals)


def filter_kernel(occ_ref, orb_ref, pot_ref, weight_ref, new_ref, send_ref, ya, yb, coef, flat):
    tiles, chunks = LX // 8, LX * LX // LANES
    line = LX + 2
    lane = iota((8, LANES), 1)
    row = iota((8, LANES), 0)
    low_z, high_z = lane % LX == 0, lane % LX == LX - 1
    first_x, last_x = row == 0, row == 7
    zero = jnp.zeros((8, LANES), F32)
    alpha = -2.0 * kinetic / half_width
    scale, shift = 2.0 / half_width, (2.0 / half_width) * (6.0 * kinetic - centre_value)

    for buffer in (ya, yb):
        for h in range(2):
            buffer[h * line] = jnp.zeros((LX, LANES), F32)
            buffer[h * line + line - 1] = jnp.zeros((LX, LANES), F32)

    def spread(c, carry):
        here = pl.ds(pl.multiple_of(c * LANES, LANES), LANES)
        for t in range(tiles):
            rows = slice(8 * t, 8 * t + 8)
            v = scale * pot_ref[rows, here] + shift
            for y in range(PER):
                value = jnp.where(lane // LX == y, v, 0.0)
                value = value + pltpu.roll(value, LX, 1)
                coef[PER * c + y, rows, :] = value + pltpu.roll(value, 2 * LX, 1)
        return carry

    lax.fori_loop(0, chunks, spread, 0)

    def advance(src, before, dst):
        def one(b, carry):
            for yy in range(GROUP):
                y = GROUP * b + yy
                for h in range(2):
                    at = h * line + 1 + y
                    cells = [src[at, 8 * t : 8 * t + 8, :] for t in range(tiles)]
                    for t in range(tiles):
                        rows = slice(8 * t, 8 * t + 8)
                        cur = cells[t]
                        above = cells[t - 1] if t > 0 else zero
                        below = cells[t + 1] if t < tiles - 1 else zero
                        total = jnp.where(low_z, zero, pltpu.roll(cur, 1, 1))
                        total += jnp.where(high_z, zero, pltpu.roll(cur, LANES - 1, 1))
                        total += pltpu.roll(jnp.where(last_x, above, cur), 1, 0)
                        total += pltpu.roll(jnp.where(first_x, below, cur), 7, 0)
                        total += src[at - 1, rows, :] + src[at + 1, rows, :]
                        result = alpha * total + coef[y, rows, :] * cur
                        if before is None:
                            dst[at, rows, :] = 0.5 * result
                        else:
                            dst[at, rows, :] = result - before[at, rows, :]
            return carry

        lax.fori_loop(0, LX // GROUP, one, 0)

    advance(orb_ref, None, yb)
    advance(yb, orb_ref, ya)

    def two(m, carry):
        advance(ya, yb, yb)
        advance(yb, ya, ya)
        return carry

    lax.fori_loop(0, (DEGREE - 2) // 2, two, 0)

    pairs = [(n, m) for n in range(NORB) for m in range(n + 1)]

    def take(c, carry):
        here = pl.ds(pl.multiple_of(c * LANES, LANES), LANES)
        for t in range(tiles):
            rows = slice(8 * t, 8 * t + 8)
            for h in range(2):
                v = [ya[h * line + 1 + PER * c + y, rows, :] for y in range(PER)]
                for g, value in enumerate(swap_four(v, lane)):
                    flat[4 * h + g, rows, here] = value
        return carry

    lax.fori_loop(0, chunks, take, 0)

    def gather(t, sums):
        sums = list(sums)
        rows = pl.ds(pl.multiple_of(8 * t, 8), 8)
        for c in range(chunks):
            f = [flat[n, rows, c * LANES : (c + 1) * LANES] for n in range(NORB)]
            for at, (n, m) in enumerate(pairs):
                sums[at] = sums[at] + f[n] * f[m]
        return tuple(sums)

    sums = lax.fori_loop(0, tiles, gather, tuple(zero for _ in pairs))
    gram = {
        pair: jnp.sum(jnp.sum(s, axis=0, keepdims=True), axis=1, keepdims=True) / float(LX**3)
        for pair, s in zip(pairs, sums)
    }
    factor, inverse, recip = {}, {}, {}
    for j in range(NORB):
        rest = gram[j, j]
        for k in range(j):
            rest = rest - factor[j, k] * factor[j, k]
        recip[j] = 1.0 / jnp.sqrt(rest)
        for n in range(j + 1, NORB):
            value = gram[n, j]
            for k in range(j):
                value = value - factor[n, k] * factor[j, k]
            factor[n, j] = value * recip[j]
    for j in range(NORB):
        inverse[j, j] = recip[j]
        for n in range(j + 1, NORB):
            value = factor[n, j] * inverse[j, j]
            for k in range(j + 1, n):
                value = value + factor[n, k] * inverse[k, j]
            inverse[n, j] = -recip[n] * value
    wide = {pair: jnp.broadcast_to(inverse[pair], (8, LANES)) for pair in pairs}

    kept = KEPT // PER
    occ = [jnp.broadcast_to(occ_ref[n : n + 1, :], (8, LANES)) for n in range(NORB)]

    def normal(t, carry):
        rows = pl.ds(pl.multiple_of(8 * t, 8), 8)
        for c in range(chunks):
            here = slice(c * LANES, (c + 1) * LANES)
            f = [flat[n, rows, here] for n in range(NORB)]
            total = zero
            for n in range(NORB):
                value = wide[n, 0] * f[0]
                for m in range(1, n + 1):
                    value = value + wide[n, m] * f[m]
                flat[n, rows, here] = value
                total = total + occ[n] * (value * value)
            if 1 <= c <= kept:
                coef[c, rows, :] = swap_inner(total * weight_ref[rows, here], row, lane)
        return carry

    lax.fori_loop(0, tiles, normal, 0)

    def finish(n, carry):
        new_ref[n] = flat[n].astype(BF16)
        return carry

    lax.fori_loop(0, NORB, finish, 0)

    for c in range(kept):
        for x in range(kept):
            value = coef[c + 1, PER * (x + 1) : PER * (x + 2), :]
            for s in range(PARTS):
                start = s * KEPT * kept + PER * c * kept + x
                send_ref[pl.ds(start, PER, stride=kept), :] = value


def filtered_set(occupations, orbitals, potential_ext):
    return call(
        filter_kernel,
        (
            jax.ShapeDtypeStruct((NORB, LX, LX * LX), BF16),
            jax.ShapeDtypeStruct((PARTS * KEPT * KEPT // PER, LANES), F32),
        ),
        [VMEM, VMEM, VMEM, VMEM],
        [
            pltpu.VMEM((2 * (LX + 2), LX, LANES), F32),
            pltpu.VMEM((2 * (LX + 2), LX, LANES), F32),
            pltpu.VMEM((LX, LX, LANES), F32),
            pltpu.VMEM((NORB, LX, LX * LX), F32),
        ],
        flops=60000000,
        name="filter",
    )(occupations, orbitals, potential_ext, jnp.asarray(WEIGHT))


def y_kernel(got_ref, high_ref, low_ref, send_ref):
    kept = KEPT // PER
    part = kept // 2
    chunk = kept + part
    at = lax.axis_index("gy")
    odd = lax.rem(lax.axis_index("gx"), 2) == 1
    table = (high_ref[at], low_ref[at])
    folded = []
    for c in range(kept):
        lines = got_ref[pl.ds(c, PARTS * KEPT, stride=kept), :]
        value = dot3(table, halves(lines))
        folded.append(value[CORE:])
        for q in range(4):
            send_ref[pl.ds(q * chunk + part + c, CORE, stride=4 * chunk), :] = value[:CORE]
    for c in range(part):
        low, high = folded[c], folded[part + c]
        send_ref[pl.ds(c, LX, stride=2 * chunk), :] = jnp.where(odd, high, low)
        send_ref[pl.ds(chunk + c, LX, stride=2 * chunk), :] = jnp.where(odd, low, high)


def along_y(got):
    return call(
        y_kernel,
        jax.ShapeDtypeStruct((64 * CHUNK, LANES), F32),
        [VMEM, VMEM, VMEM],
        name="along_y",
    )(got, *map(jnp.asarray, TABLES["along"]))


def plane_kernel(
    got_ref,
    zh_ref,
    zl_ref,
    yh_ref,
    yl_ref,
    wave_ref,
    own_ref,
    bh_ref,
    bl_ref,
    th_ref,
    tl_ref,
    send_ref,
    work,
):
    kept = KEPT // PER
    part = kept // 2
    chunk = kept + part
    out_chunk = 6
    wide = PARTS * LANES
    blocks = []
    for k in range(PARTS):
        rows = [
            got_ref[pl.ds(chunk * k + part + c, PARTS, stride=chunk * PARTS), :]
            for c in range(kept)
        ]
        blocks.append(jnp.concatenate(rows, axis=0))
    lines = jnp.concatenate(blocks, axis=1)
    which = (iota(lines.shape, 1) % LANES) // LX
    spread = jnp.concatenate([jnp.where(which == y, lines, 0.0) for y in range(PER)], axis=0)
    along_z = dot3(halves(spread), (zh_ref[...], zl_ref[...]))
    spectrum = dot3((yh_ref[...], yl_ref[...]), halves(along_z))
    member = lax.axis_index("gx") * PARTS + lax.axis_index("gz")
    number = lax.axis_index("gy") * CORE + lax.div(member, 4)
    eigen = wave_ref[...] + own_ref[pl.ds(number, 1), :]
    positive = eigen > 0.0
    green = jnp.where(positive, 4.0 * math.pi / jnp.where(positive, eigen, 1.0), 0.0)
    spectrum = spectrum * green
    quarter = lax.rem(member, 4)
    lines = dot3((bh_ref[quarter], bl_ref[quarter]), halves(spectrum))
    spread = dot3(halves(lines), (th_ref[...], tl_ref[...]))
    which = (iota((16, wide), 1) % LANES) // LX
    packed = jnp.zeros((16, wide), F32)
    for y in range(PER):
        packed = jnp.where(which == y, spread[16 * y : 16 * (y + 1)], packed)
    for k in range(PARTS):
        for half in range(2):
            send_ref[pl.ds(out_chunk * k + half, PARTS, stride=out_chunk * PARTS), :] = packed[
                8 * half : 8 * half + 8, k * LANES : (k + 1) * LANES
            ]
    row = iota((8, LANES), 0)
    left = iota((8, LANES), 1) % LX < LX // 2
    half = LX // 2
    first, second = row < part, lax.rem(member, 2) == 1

    def load(i, k):
        at = chunk * (PARTS * i + k)
        return jnp.where(first, got_ref[at : at + 8, :], 0.0)

    for k in range(PARTS):
        column = [load(i, k) for i in range(PARTS)]
        for m in range(PARTS):
            at = 8 * (PARTS * m + k)
            work[at : at + 8, :] = pltpu.roll(column[m], 1, 0) + column[m - 1]
    for m in range(PARTS):
        after = (m + 1) % PARTS
        other = second if m % 2 == 0 else jnp.logical_not(second)
        line = []
        for k in range(PARTS):
            here, there = 8 * (PARTS * m + k), 8 * (PARTS * after + k)
            line.append(jnp.where(other, work[there : there + 8, :], work[here : here + 8, :]))
        for k in range(PARTS):
            beside = jnp.where(left, line[(k + 1) % PARTS], line[(k - 1) % PARTS])
            value = line[k] + jnp.where(
                left, pltpu.roll(beside, LANES - half, 1), pltpu.roll(beside, half, 1)
            )
            at = out_chunk * (PARTS * m + k) + 2
            send_ref[at : at + 4, :] = value[0:4]


def on_plane(got):
    t = TABLES
    return call(
        plane_kernel,
        jax.ShapeDtypeStruct((64 * 6, LANES), F32),
        [VMEM] * 11,
        [pltpu.VMEM((64 * 8, LANES), F32)],
        name="on_plane",
    )(
        got,
        *map(jnp.asarray, t["z_table"]),
        *map(jnp.asarray, t["y_table"]),
        jnp.asarray(t["wave_yz"]),
        jnp.asarray(t["wave"]),
        *map(jnp.asarray, t["y_back"]),
        *map(jnp.asarray, t["z_back"]),
    )


def cube_root(value):
    safe = jnp.maximum(value, 1e-30)
    root = jnp.exp(jnp.log(safe) * (1.0 / 3.0))
    root = root - (root - safe / (root * root)) * (1.0 / 3.0)
    return jnp.where(value > 0.0, root, 0.0)


def exchange_correlation(density):
    root = cube_root(density)
    slater = -((3.0 / math.pi) ** (1.0 / 3.0)) * root
    radius = (3.0 / (4.0 * math.pi)) ** (1.0 / 3.0)
    bottom = radius + 7.8 * root
    wigner = -0.44 * root / bottom * (1.0 + radius / (3.0 * bottom))
    return slater + wigner


def window_kernel(got_ref, ion_ref, send_ref, dens_ref, base_ref, work):
    for half in range(2):
        value = got_ref[pl.ds(half, 64, stride=6), :]
        for s in range(PARTS):
            send_ref[pl.ds(s * LANES + half, 64, stride=2), :] = value
    row, lane = iota((8, LANES), 0), iota((8, LANES), 1)
    odd = lax.rem(lax.axis_index("gx"), 2) == 1
    for q in range(2):
        for h in range(4):
            x = 4 * q + h
            value = jnp.where(
                odd,
                got_ref[pl.ds(6 * (1 - q) + 2 + h, LX, stride=12), :],
                got_ref[pl.ds(6 * q + 2 + h, LX, stride=12), :],
            )
            if 2 <= x < 6:
                for low in range(PER):
                    core = pltpu.roll(value[BUF : BUF + CORE], LANES - LX * low - BUF, 1)
                    dens_ref[PER * (x - 2) + low] = core[:, :CORE]
            for t in range(4):
                piece = swap_inner(value[8 * t : 8 * t + 8], row, lane)
                for half in range(2):
                    y = 2 * t + half
                    work[PER * x : PER * x + PER, y * LANES : (y + 1) * LANES] = piece[
                        PER * half : PER * half + PER
                    ]
    base_ref[...] = ion_ref[...] + exchange_correlation(work[...])


def on_window(got, ion_ext):
    return call(
        window_kernel,
        (
            jax.ShapeDtypeStruct((PARTS * LANES, LANES), F32),
            jax.ShapeDtypeStruct((CORE, CORE, CORE), F32),
            jax.ShapeDtypeStruct((LX, LX * LX), F32),
        ),
        [VMEM, VMEM],
        [pltpu.VMEM((LX, LX * LX), F32)],
        name="on_window",
    )(got, ion_ext)


def last_kernel(got_ref, base_ref, high_ref, low_ref, out_ref):
    at = lax.axis_index("gy")
    table = (high_ref[at], low_ref[at])
    row, lane = iota((8, LANES), 0), iota((8, LANES), 1)
    for x in range(8):
        lines = got_ref[pl.ds(x, N, stride=8), :]
        value = dot3(table, halves(lines))
        rows = slice(PER * x, PER * x + PER)
        for t in range(4):
            piece = swap_inner(value[8 * t : 8 * t + 8], row, lane)
            for half in range(2):
                y = 2 * t + half
                here = slice(y * LANES, (y + 1) * LANES)
                out_ref[rows, here] = base_ref[rows, here] + piece[PER * half : PER * half + PER]


def last_step(got, base):
    return call(
        last_kernel,
        jax.ShapeDtypeStruct((LX, LX * LX), F32),
        [VMEM, VMEM, VMEM, VMEM],
        name="last_step",
    )(got, base, *map(jnp.asarray, TABLES["last"]))


def both_sides(first, last, axis):
    count = lax.axis_size(axis)
    up = [(i, (i + 1) % count) for i in range(count)]
    down = [(j, i) for i, j in up]
    return lax.ppermute(last, axis, up), lax.ppermute(first, axis, down)


def pack_kernel(pot_hbm, ion_hbm, own_ref, up_ref, down_ref, pot_ref, ion_ref, sems):
    copies = [
        pltpu.make_async_copy(source, target, sems.at[f])
        for f, (source, target) in enumerate(((pot_hbm, pot_ref), (ion_hbm, ion_ref)))
    ]
    for copy in copies:
        copy.start()
    for copy in copies:
        copy.wait()
    lane = iota((CORE, LANES), 1)
    third = (lane % LX) // BUF
    for f, ref in enumerate((pot_ref, ion_ref)):
        rows = slice(CORE * f, CORE * (f + 1))
        up, down = jnp.zeros((CORE, LANES), F32), jnp.zeros((CORE, LANES), F32)
        for c in range(PER):
            value = jnp.zeros((CORE, LANES), F32)
            for y in range(PER):
                line = ref[pl.ds(PER * c + y, CORE, stride=CORE), :]
                line = jnp.concatenate([line, jnp.zeros((CORE, LANES - CORE), F32)], axis=1)
                value = value + pltpu.roll(line, LX * y + BUF, 1)
            own_ref[rows, c * LANES : (c + 1) * LANES] = value
            up = jnp.where(third == c, pltpu.roll(value, (BUF * c - 2 * BUF) % LANES, 1), up)
            down = jnp.where(third == c, pltpu.roll(value, (BUF * c - BUF) % LANES, 1), down)
        up_ref[rows, :] = up
        down_ref[rows, :] = down


def merge_kernel(own_ref, before_ref, after_ref, out_ref):
    third = (iota((2 * CORE, LANES), 1) % LX) // BUF
    before, after = before_ref[...], after_ref[...]
    for c in range(PER):
        here = slice(c * LANES, (c + 1) * LANES)
        value = jnp.where(third == 0, pltpu.roll(before, (-BUF * c) % LANES, 1), own_ref[:, here])
        out_ref[:, here] = jnp.where(
            third == 3, pltpu.roll(after, (3 * BUF - BUF * c) % LANES, 1), value
        )


def refill(potential, ion_potential, orbitals, wide_occ):
    fields = 2
    count = fields * CORE
    slab = jax.ShapeDtypeStruct((count, LANES), F32)
    full = jax.ShapeDtypeStruct((count, CORE * LX), F32)
    lines = pltpu.VMEM((CORE * CORE, CORE), F32)
    scratch = [lines, lines, pltpu.SemaphoreType.DMA((2,))]
    own, up, down = call(pack_kernel, (full, slab, slab), [HBM, HBM], scratch, name="pack")(
        *[f.reshape(CORE * CORE, CORE) for f in (potential, ion_potential)]
    )
    before, after = both_sides(down, up, "gz")
    both = call(merge_kernel, full, [VMEM, VMEM, VMEM], name="merge")(own, before, after)
    width = BUF * LX
    before, after = both_sides(both[:, :width], both[:, CORE * LX - width :], "gy")
    both = jnp.concatenate([before, both, after], axis=1).reshape(fields, CORE, LX * LX)
    both, orbitals, wide_occ = lax.optimization_barrier((both, orbitals, wide_occ))
    before, after = both_sides(both[:, :BUF], both[:, CORE - BUF :], "gx")
    brought = bring_orbitals(orbitals)
    whole = jnp.concatenate([before, both, after], axis=1)
    return whole[0], whole[1], brought, wide_occ


def exchange(value, axis, rows):
    parts = value.shape[0] // rows
    tile = math.gcd(rows, 8)
    shaped = value.reshape(value.shape[0] // tile, tile, LANES)
    return lax.all_to_all(shaped, axis, split_axis=0, concat_axis=0, tiled=True).reshape(
        value.shape
    )


def on_device(orbitals, potential, ion_potential, occupations):
    wide_occ = jnp.broadcast_to(occupations[:, None], (NORB, LANES))
    pot_ext, ion_ext, brought, wide_occ = refill(potential, ion_potential, orbitals, wide_occ)
    new_orbitals, send = filtered_set(wide_occ, brought, pot_ext)
    got = exchange(send, "gy", KEPT * KEPT // PER)
    send = along_y(got)
    got = exchange(send, ("gx", "gz"), CHUNK)
    send = on_plane(got)
    got = exchange(send, ("gx", "gz"), 6)
    send, density, base = on_window(got, ion_ext)
    got = exchange(send, "gy", LANES)
    new_potential = last_step(got, base)
    return (new_orbitals, density, new_potential)


def solution(mesh):
    placed = (P(None, "gx", ("gy", "gz")), P("gx", "gy", "gz"), P("gx", "gy", "gz"), P())
    return jax.shard_map(
        on_device,
        mesh=mesh,
        in_specs=placed,
        out_specs=(P(None, "gx", ("gy", "gz")), P("gx", "gy", "gz"), P("gx", ("gy", "gz"))),
        check_vma=False,
    )
```

```python
import functools
import math

import jax
import jax.numpy as jnp
import numpy as np
from jax import lax
from jax.experimental import pallas as pl
from jax.experimental.pallas import tpu as pltpu
from jax.sharding import PartitionSpec as P

BUF = 8
DEGREE = 10
N = 128
CORE = 16
LX = 32
NORB = 8
PARTS = 8
FIRST, LAST = 4, 28
KEPT = LAST - FIRST
LANES = 128
CHUNK = 7
GROUP = 16
PER = LANES // LX

spacing = 0.2
kinetic = 0.5 / (spacing * spacing)
filter_low = 6.0
filter_high = 12.0 * kinetic
centre_value = 0.5 * (filter_low + filter_high)
half_width = 0.5 * (filter_high - filter_low)

F32, BF16 = jnp.float32, jnp.bfloat16
VMEM = pl.BlockSpec(memory_space=pltpu.VMEM)
SMEM = pl.BlockSpec(memory_space=pltpu.SMEM)
INTERPRET = False


def call(kernel, out_shape, in_specs, scratch=(), flops=1000000, name=None):
    many = isinstance(out_shape, (tuple, list))
    return pl.pallas_call(
        kernel,
        out_shape=out_shape,
        in_specs=in_specs,
        out_specs=tuple(VMEM for _ in out_shape) if many else VMEM,
        scratch_shapes=scratch,
        compiler_params=pltpu.CompilerParams(vmem_limit_bytes=40 * 1024 * 1024),
        cost_estimate=pl.CostEstimate(flops=flops, bytes_accessed=1000000, transcendentals=0),
        interpret=INTERPRET,
        name=name,
    )


def _basis():
    n = np.arange(N, dtype=np.float64)
    angle = 2.0 * np.pi * np.mod(np.outer(n, n), N) / N
    return (np.cos(angle) + np.sin(angle)) / math.sqrt(N)


def _pair(table):
    high = np.asarray(table, np.float32).astype(jnp.bfloat16)
    low = (np.asarray(table, np.float64) - high.astype(np.float64)).astype(jnp.bfloat16)
    return high, low


def _cell(part, a):
    return np.mod(CORE * part + a - BUF, N)


def _tables():
    basis = _basis()
    parts = np.arange(PARTS)
    along = np.zeros((PARTS, CORE + LX, PARTS * KEPT))
    for i in range(PARTS):
        for other in range(PARTS):
            for xx in range(KEPT):
                column = other * KEPT + xx
                cell = _cell(other, xx + FIRST)
                along[i, :CORE, column] = basis[CORE * i : CORE * (i + 1), cell]
                for a in range(LX):
                    if _cell(i, a) == cell and min((other - i) % PARTS, (i - other) % PARTS) <= 1:
                        along[i, CORE + (a % 2) * CORE + a // 2, column] = 1.0
    lane = np.arange(PARTS * LANES)
    z_cell = _cell(lane // LANES, lane % LX)
    z_table = basis[z_cell, :]
    y_lo, y_hi, j = np.meshgrid(np.arange(PER), np.arange(KEPT // PER), parts, indexing="ij")
    y_table = basis[:, _cell(j, FIRST + PER * y_hi + y_lo).reshape(-1)]
    back = np.zeros((4, 64, N))
    for q in range(4):
        y_lo, y_half, j = np.meshgrid(np.arange(PER), np.arange(2), parts, indexing="ij")
        back[q] = basis[_cell(j, 8 * q + PER * y_half + y_lo).reshape(-1), :]
    last = np.stack([basis[_cell(i, np.arange(LX)), :] for i in range(PARTS)])
    wave = 4.0 / (spacing * spacing) * np.sin(np.pi * np.arange(N) / N) ** 2
    return dict(
        along=_pair(along),
        z_table=_pair(z_table),
        z_back=_pair(z_table.T),
        y_table=_pair(y_table),
        y_back=_pair(back),
        last=_pair(last),
        wave=np.repeat(wave.astype(np.float32)[:, None], LANES, axis=1),
        wave_yz=(wave[:, None] + wave[None, :]).astype(np.float32),
    )


def _weight():
    position = np.arange(LX, dtype=np.float32)
    rising = np.clip((position + 0.5 - 0.5 * BUF) / BUF, 0.0, 1.0)
    falling = np.clip((LX - 0.5 * BUF - 0.5 - position) / BUF, 0.0, 1.0)
    profile = (rising * falling).astype(np.float32)
    return profile[:, None] * (profile[:, None] * profile[None, :]).reshape(1, LX * LX)


TABLES = _tables()
WEIGHT = _weight().astype(np.float32)


def halves(value):
    high = value.astype(BF16)
    return high, (value - high.astype(F32)).astype(BF16)


def dot3(left, right):
    def one(a, b):
        return jnp.dot(a, b, preferred_element_type=F32)

    return one(left[0], right[0]) + (one(left[0], right[1]) + one(left[1], right[0]))


def iota(shape, dim):
    return lax.broadcasted_iota(jnp.int32, shape, dim)


def swap_four(v, lane):
    low, even = lane < 2 * LX, (lane // LX) % 2 == 0
    w = [None] * 4
    for g in range(2):
        w[g] = jnp.where(low, v[g], pltpu.roll(v[g + 2], 2 * LX, 1))
        w[g + 2] = jnp.where(low, pltpu.roll(v[g], 2 * LX, 1), v[g + 2])
    out = []
    for g in (0, 2):
        out.append(jnp.where(even, w[g], pltpu.roll(w[g + 1], LX, 1)))
        out.append(jnp.where(even, pltpu.roll(w[g], 3 * LX, 1), w[g + 1]))
    return out


def swap_inner(v, row, lane):
    a, b = row % 4, lane // LX
    turned = pltpu.roll(v, 2 * LX, 1)
    v = jnp.where(
        a // 2 == b // 2,
        v,
        jnp.where(a < 2, pltpu.roll(turned, 6, 0), pltpu.roll(turned, 2, 0)),
    )
    return jnp.where(
        a % 2 == b % 2,
        v,
        jnp.where(
            a % 2 == 0,
            pltpu.roll(pltpu.roll(v, LX, 1), 7, 0),
            pltpu.roll(pltpu.roll(v, 3 * LX, 1), 1, 0),
        ),
    )


def bring_kernel(occ_ref, orb_ref, out_ref, wide_ref):
    tiles, chunks = LX // 8, LX * LX // LANES
    lane = iota((8, LANES), 1)
    line = LX + 2
    for n in range(NORB):
        wide_ref[n : n + 1, :] = jnp.full((1, LANES), occ_ref[n], F32)
    for h in range(2):
        out_ref[h * line] = jnp.zeros((LX, LANES), F32)
        out_ref[h * line + line - 1] = jnp.zeros((LX, LANES), F32)

    def bring(c, carry):
        here = pl.ds(pl.multiple_of(c * LANES, LANES), LANES)
        for t in range(tiles):
            rows = slice(8 * t, 8 * t + 8)
            for h in range(2):
                v = [orb_ref[4 * h + g, rows, here].astype(F32) for g in range(4)]
                for y, value in enumerate(swap_four(v, lane)):
                    out_ref[h * line + 1 + PER * c + y, rows, :] = value
        return carry

    lax.fori_loop(0, chunks, bring, 0)


def bring_orbitals(occupations, orbitals):
    return call(
        bring_kernel,
        (
            jax.ShapeDtypeStruct((2 * (LX + 2), LX, LANES), F32),
            jax.ShapeDtypeStruct((NORB, LANES), F32),
        ),
        [SMEM, VMEM],
        flops=15000000,
        name="bring",
    )(occupations, orbitals)


def filter_kernel(occ_ref, orb_ref, pot_ref, weight_ref, new_ref, send_ref, ya, yb, coef, flat):
    tiles, chunks = LX // 8, LX * LX // LANES
    line = LX + 2
    lane = iota((8, LANES), 1)
    row = iota((8, LANES), 0)
    low_z, high_z = lane % LX == 0, lane % LX == LX - 1
    first_x, last_x = row == 0, row == 7
    zero = jnp.zeros((8, LANES), F32)
    alpha = -2.0 * kinetic / half_width
    scale, shift = 2.0 / half_width, (2.0 / half_width) * (6.0 * kinetic - centre_value)

    for buffer in (ya, yb):
        for h in range(2):
            buffer[h * line] = jnp.zeros((LX, LANES), F32)
            buffer[h * line + line - 1] = jnp.zeros((LX, LANES), F32)

    def spread(c, carry):
        here = pl.ds(pl.multiple_of(c * LANES, LANES), LANES)
        for t in range(tiles):
            rows = slice(8 * t, 8 * t + 8)
            v = scale * pot_ref[rows, here] + shift
            for y in range(PER):
                value = jnp.where(lane // LX == y, v, 0.0)
                value = value + pltpu.roll(value, LX, 1)
                coef[PER * c + y, rows, :] = value + pltpu.roll(value, 2 * LX, 1)
        return carry

    lax.fori_loop(0, chunks, spread, 0)

    def advance(src, before, dst):
        def one(b, carry):
            for yy in range(GROUP):
                y = GROUP * b + yy
                for h in range(2):
                    at = h * line + 1 + y
                    cells = [src[at, 8 * t : 8 * t + 8, :] for t in range(tiles)]
                    for t in range(tiles):
                        rows = slice(8 * t, 8 * t + 8)
                        cur = cells[t]
                        above = cells[t - 1] if t > 0 else zero
                        below = cells[t + 1] if t < tiles - 1 else zero
                        total = jnp.where(low_z, zero, pltpu.roll(cur, 1, 1))
                        total += jnp.where(high_z, zero, pltpu.roll(cur, LANES - 1, 1))
                        total += pltpu.roll(jnp.where(last_x, above, cur), 1, 0)
                        total += pltpu.roll(jnp.where(first_x, below, cur), 7, 0)
                        total += src[at - 1, rows, :] + src[at + 1, rows, :]
                        result = alpha * total + coef[y, rows, :] * cur
                        if before is None:
                            dst[at, rows, :] = 0.5 * result
                        else:
                            dst[at, rows, :] = result - before[at, rows, :]
            return carry

        lax.fori_loop(0, LX // GROUP, one, 0)

    advance(orb_ref, None, yb)
    advance(yb, orb_ref, ya)

    def two(m, carry):
        advance(ya, yb, yb)
        advance(yb, ya, ya)
        return carry

    lax.fori_loop(0, (DEGREE - 2) // 2, two, 0)

    pairs = [(n, m) for n in range(NORB) for m in range(n + 1)]

    def take(c, carry):
        here = pl.ds(pl.multiple_of(c * LANES, LANES), LANES)
        for t in range(tiles):
            rows = slice(8 * t, 8 * t + 8)
            for h in range(2):
                v = [ya[h * line + 1 + PER * c + y, rows, :] for y in range(PER)]
                for g, value in enumerate(swap_four(v, lane)):
                    flat[4 * h + g, rows, here] = value
        return carry

    lax.fori_loop(0, chunks, take, 0)

    def gather(t, sums):
        sums = list(sums)
        rows = pl.ds(pl.multiple_of(8 * t, 8), 8)
        for c in range(chunks):
            f = [flat[n, rows, c * LANES : (c + 1) * LANES] for n in range(NORB)]
            for at, (n, m) in enumerate(pairs):
                sums[at] = sums[at] + f[n] * f[m]
        return tuple(sums)

    sums = lax.fori_loop(0, tiles, gather, tuple(zero for _ in pairs))
    gram = {
        pair: jnp.sum(jnp.sum(s, axis=0, keepdims=True), axis=1, keepdims=True) / float(LX**3)
        for pair, s in zip(pairs, sums)
    }
    factor, inverse, recip = {}, {}, {}
    for j in range(NORB):
        rest = gram[j, j]
        for k in range(j):
            rest = rest - factor[j, k] * factor[j, k]
        recip[j] = 1.0 / jnp.sqrt(rest)
        for n in range(j + 1, NORB):
            value = gram[n, j]
            for k in range(j):
                value = value - factor[n, k] * factor[j, k]
            factor[n, j] = value * recip[j]
    for j in range(NORB):
        inverse[j, j] = recip[j]
        for n in range(j + 1, NORB):
            value = factor[n, j] * inverse[j, j]
            for k in range(j + 1, n):
                value = value + factor[n, k] * inverse[k, j]
            inverse[n, j] = -recip[n] * value
    wide = {pair: jnp.broadcast_to(inverse[pair], (8, LANES)) for pair in pairs}

    kept = KEPT // PER
    occ = [jnp.broadcast_to(occ_ref[n : n + 1, :], (8, LANES)) for n in range(NORB)]

    def normal(t, carry):
        rows = pl.ds(pl.multiple_of(8 * t, 8), 8)
        for c in range(chunks):
            here = slice(c * LANES, (c + 1) * LANES)
            f = [flat[n, rows, here] for n in range(NORB)]
            total = zero
            for n in range(NORB):
                value = wide[n, 0] * f[0]
                for m in range(1, n + 1):
                    value = value + wide[n, m] * f[m]
                flat[n, rows, here] = value
                total = total + occ[n] * (value * value)
            if 1 <= c <= kept:
                coef[c, rows, :] = swap_inner(total * weight_ref[rows, here], row, lane)
        return carry

    lax.fori_loop(0, tiles, normal, 0)

    def finish(n, carry):
        new_ref[n] = flat[n].astype(BF16)
        return carry

    lax.fori_loop(0, NORB, finish, 0)

    for c in range(kept):
        for x in range(kept):
            value = coef[c + 1, PER * (x + 1) : PER * (x + 2), :]
            for s in range(PARTS):
                start = s * KEPT * kept + PER * c * kept + x
                send_ref[pl.ds(start, PER, stride=kept), :] = value


def filtered_set(occupations, orbitals, potential_ext):
    return call(
        filter_kernel,
        (
            jax.ShapeDtypeStruct((NORB, LX, LX * LX), BF16),
            jax.ShapeDtypeStruct((PARTS * KEPT * KEPT // PER, LANES), F32),
        ),
        [VMEM, VMEM, VMEM, VMEM],
        [
            pltpu.VMEM((2 * (LX + 2), LX, LANES), F32),
            pltpu.VMEM((2 * (LX + 2), LX, LANES), F32),
            pltpu.VMEM((LX, LX, LANES), F32),
            pltpu.VMEM((NORB, LX, LX * LX), F32),
        ],
        flops=60000000,
        name="filter",
    )(occupations, orbitals, potential_ext, jnp.asarray(WEIGHT))


def crop(value, lane):
    out = pltpu.roll(value, LANES - FIRST, 1)
    for x in range(1, PER):
        moved = pltpu.roll(value, LANES - FIRST - 8 * x, 1)
        out = jnp.where(lane < KEPT * x, out, moved)
    return out


def uncrop(value, lane):
    out = jnp.zeros_like(value)
    inside = (lane % LX >= FIRST) & (lane % LX < LAST)
    for x in range(PER):
        here = inside & (lane // LX == x)
        out = jnp.where(here, pltpu.roll(value, FIRST + 8 * x, 1), out)
    return out


def y_kernel(got_ref, high_ref, low_ref, send_ref):
    kept = KEPT // PER
    part = kept // 2
    at = lax.axis_index("gy")
    odd = lax.rem(lax.axis_index("gx"), 2) == 1
    lane = iota((CORE, LANES), 1)
    table = (high_ref[at], low_ref[at])
    waves, folded = [], ([], [])
    for c in range(kept):
        lines = got_ref[pl.ds(c, PARTS * KEPT, stride=kept), :]
        value = dot3(table, halves(lines))
        waves.append(crop(value[:CORE], lane))
        for s in range(2):
            folded[s].append(crop(value[CORE * (1 + s) : CORE * (2 + s)], lane))
    for q in range(4):
        planes = folded[q // 2]
        thirds = []
        for c in range(part):
            low, high = planes[c], planes[part + c]
            first, second = (low, high) if q % 2 == 0 else (high, low)
            thirds.append(jnp.where(odd, second, first))
        for c in range(kept):
            piece = pltpu.roll(thirds[1 + c // part], 3 * LX - LX * (c % part), 1)
            row = jnp.where(lane < 3 * LX, waves[c], piece)
            send_ref[pl.ds(q * CHUNK + c, CORE, stride=4 * CHUNK), :] = row
        send_ref[pl.ds(q * CHUNK + kept, CORE, stride=4 * CHUNK), :] = thirds[0]


def along_y(got):
    return call(
        y_kernel,
        jax.ShapeDtypeStruct((64 * CHUNK, LANES), F32),
        [VMEM, VMEM, VMEM],
        name="along_y",
    )(got, *map(jnp.asarray, TABLES["along"]))


def plane_kernel(
    got_ref,
    zh_ref,
    zl_ref,
    yh_ref,
    yl_ref,
    wave_ref,
    own_ref,
    bh_ref,
    bl_ref,
    th_ref,
    tl_ref,
    send_ref,
):
    kept = KEPT // PER
    part = kept // 2
    out_chunk = 6
    wide = PARTS * LANES
    lane = iota((PARTS, LANES), 1)
    blocks, thirds = [], []
    for k in range(PARTS):
        rows = [got_ref[pl.ds(CHUNK * k + c, PARTS, stride=CHUNK * PARTS), :] for c in range(CHUNK)]
        blocks.append(jnp.concatenate([uncrop(rows[c], lane) for c in range(kept)], axis=0))
        units = [rows[kept]]
        for u in range(2):
            unit = pltpu.roll(rows[part * u], LX, 1)
            for c in range(1, part):
                moved = pltpu.roll(rows[part * u + c], LX + LX * c, 1)
                unit = jnp.where(lane < LX * c, unit, moved)
            units.append(unit)
        thirds.append([uncrop(unit, lane) for unit in units])
    lines = jnp.concatenate(blocks, axis=1)
    which = (iota(lines.shape, 1) % LANES) // LX
    spread = jnp.concatenate([jnp.where(which == y, lines, 0.0) for y in range(PER)], axis=0)
    along_z = dot3(halves(spread), (zh_ref[...], zl_ref[...]))
    spectrum = dot3((yh_ref[...], yl_ref[...]), halves(along_z))
    member = lax.axis_index("gx") * PARTS + lax.axis_index("gz")
    number = lax.axis_index("gy") * CORE + lax.div(member, 4)
    eigen = wave_ref[...] + own_ref[pl.ds(number, 1), :]
    positive = eigen > 0.0
    green = jnp.where(positive, 4.0 * math.pi / jnp.where(positive, eigen, 1.0), 0.0)
    spectrum = spectrum * green
    quarter = lax.rem(member, 4)
    lines = dot3((bh_ref[quarter], bl_ref[quarter]), halves(spectrum))
    spread = dot3(halves(lines), (th_ref[...], tl_ref[...]))
    which = (iota((16, wide), 1) % LANES) // LX
    packed = jnp.zeros((16, wide), F32)
    for y in range(PER):
        packed = jnp.where(which == y, spread[16 * y : 16 * (y + 1)], packed)
    for k in range(PARTS):
        for half in range(2):
            send_ref[pl.ds(out_chunk * k + half, PARTS, stride=out_chunk * PARTS), :] = packed[
                8 * half : 8 * half + 8, k * LANES : (k + 1) * LANES
            ]
    left = lane % LX < LX // 2
    half = LX // 2
    own = iota((PARTS, LANES), 0) % 2 == lax.rem(member, 2)
    for h in range(4):
        line = []
        for k in range(PARTS):
            if h == 0:
                line.append(pltpu.roll(thirds[k][0], 1, 0))
            elif h == part:
                line.append(thirds[k][part - 1])
            else:
                line.append(thirds[k][h - 1] + pltpu.roll(thirds[k][h], 1, 0))
        for k in range(PARTS):
            beside = jnp.where(left, line[(k + 1) % PARTS], line[(k - 1) % PARTS])
            value = line[k] + jnp.where(
                left, pltpu.roll(beside, LANES - half, 1), pltpu.roll(beside, half, 1)
            )
            value = jnp.where(own, value, pltpu.roll(value, PARTS - 1, 0))
            send_ref[pl.ds(out_chunk * k + 2 + h, PARTS, stride=out_chunk * PARTS), :] = value


def on_plane(got):
    t = TABLES
    return call(
        plane_kernel,
        jax.ShapeDtypeStruct((64 * 6, LANES), F32),
        [VMEM] * 11,
        name="on_plane",
    )(
        got,
        *map(jnp.asarray, t["z_table"]),
        *map(jnp.asarray, t["y_table"]),
        jnp.asarray(t["wave_yz"]),
        jnp.asarray(t["wave"]),
        *map(jnp.asarray, t["y_back"]),
        *map(jnp.asarray, t["z_back"]),
    )


def cube_root(value):
    safe = jnp.maximum(value, 1e-30)
    root = jnp.exp(jnp.log(safe) * (1.0 / 3.0))
    root = root - (root - safe / (root * root)) * (1.0 / 3.0)
    return jnp.where(value > 0.0, root, 0.0)


def exchange_correlation(density):
    root = cube_root(density)
    slater = -((3.0 / math.pi) ** (1.0 / 3.0)) * root
    radius = (3.0 / (4.0 * math.pi)) ** (1.0 / 3.0)
    bottom = radius + 7.8 * root
    wigner = -0.44 * root / bottom * (1.0 + radius / (3.0 * bottom))
    return slater + wigner


def window_kernel(got_ref, ion_ref, send_ref, dens_ref, base_ref, work):
    for half in range(2):
        value = got_ref[pl.ds(half, 64, stride=6), :]
        for s in range(PARTS):
            send_ref[pl.ds(s * LANES + half, 64, stride=2), :] = value
    row, lane = iota((8, LANES), 0), iota((8, LANES), 1)
    odd = lax.rem(lax.axis_index("gx"), 2) == 1
    for q in range(2):
        for h in range(4):
            x = 4 * q + h
            value = jnp.where(
                odd,
                got_ref[pl.ds(6 * (1 - q) + 2 + h, LX, stride=12), :],
                got_ref[pl.ds(6 * q + 2 + h, LX, stride=12), :],
            )
            if 2 <= x < 6:
                for low in range(PER):
                    core = pltpu.roll(value[BUF : BUF + CORE], LANES - LX * low - BUF, 1)
                    dens_ref[PER * (x - 2) + low] = core[:, :CORE]
            for t in range(4):
                piece = swap_inner(value[8 * t : 8 * t + 8], row, lane)
                for half in range(2):
                    y = 2 * t + half
                    work[PER * x : PER * x + PER, y * LANES : (y + 1) * LANES] = piece[
                        PER * half : PER * half + PER
                    ]
    base_ref[...] = ion_ref[...] + exchange_correlation(work[...])


def on_window(got, ion_ext):
    return call(
        window_kernel,
        (
            jax.ShapeDtypeStruct((PARTS * LANES, LANES), F32),
            jax.ShapeDtypeStruct((CORE, CORE, CORE), F32),
            jax.ShapeDtypeStruct((LX, LX * LX), F32),
        ),
        [VMEM, VMEM],
        [pltpu.VMEM((LX, LX * LX), F32)],
        name="on_window",
    )(got, ion_ext)


def last_kernel(got_ref, base_ref, high_ref, low_ref, out_ref):
    at = lax.axis_index("gy")
    table = (high_ref[at], low_ref[at])
    row, lane = iota((8, LANES), 0), iota((8, LANES), 1)
    for x in range(8):
        lines = got_ref[pl.ds(x, N, stride=8), :]
        value = dot3(table, halves(lines))
        rows = slice(PER * x, PER * x + PER)
        for t in range(4):
            piece = swap_inner(value[8 * t : 8 * t + 8], row, lane)
            for half in range(2):
                y = 2 * t + half
                here = slice(y * LANES, (y + 1) * LANES)
                out_ref[rows, here] = base_ref[rows, here] + piece[PER * half : PER * half + PER]


def last_step(got, base):
    return call(
        last_kernel,
        jax.ShapeDtypeStruct((LX, LX * LX), F32),
        [VMEM, VMEM, VMEM, VMEM],
        name="last_step",
    )(got, base, *map(jnp.asarray, TABLES["last"]))


def both_sides(first, last, axis):
    count = lax.axis_size(axis)
    up = [(i, (i + 1) % count) for i in range(count)]
    down = [(j, i) for i, j in up]
    return lax.ppermute(last, axis, up), lax.ppermute(first, axis, down)


def pack_kernel(fields_ref, own_ref, up_ref, down_ref):
    lane = iota((CORE, LANES), 1)
    third = (lane % LX) // BUF
    for f in range(2):
        rows = slice(CORE * f, CORE * (f + 1))
        up, down = jnp.zeros((CORE, LANES), F32), jnp.zeros((CORE, LANES), F32)
        for c in range(PER):
            value = jnp.zeros((CORE, LANES), F32)
            for y in range(PER):
                line = fields_ref[pl.ds(f * CORE * CORE + PER * c + y, CORE, stride=CORE), :]
                line = jnp.concatenate([line, jnp.zeros((CORE, LANES - CORE), F32)], axis=1)
                value = value + pltpu.roll(line, LX * y + BUF, 1)
            own_ref[rows, c * LANES : (c + 1) * LANES] = value
            up = jnp.where(third == c, pltpu.roll(value, (BUF * c - 2 * BUF) % LANES, 1), up)
            down = jnp.where(third == c, pltpu.roll(value, (BUF * c - BUF) % LANES, 1), down)
        up_ref[rows, :] = up
        down_ref[rows, :] = down


def merge_kernel(own_ref, before_ref, after_ref, out_ref):
    third = (iota((2 * CORE, LANES), 1) % LX) // BUF
    before, after = before_ref[...], after_ref[...]
    for c in range(PER):
        here = slice(c * LANES, (c + 1) * LANES)
        value = jnp.where(third == 0, pltpu.roll(before, (-BUF * c) % LANES, 1), own_ref[:, here])
        out_ref[:, here] = jnp.where(
            third == 3, pltpu.roll(after, (3 * BUF - BUF * c) % LANES, 1), value
        )


def refill(potential, ion_potential, orbitals, occupations):
    fields = 2
    count = fields * CORE
    slab = jax.ShapeDtypeStruct((count, LANES), F32)
    full = jax.ShapeDtypeStruct((count, CORE * LX), F32)
    lines = jnp.concatenate([potential, ion_potential]).reshape(fields * CORE * CORE, CORE)
    own, up, down = call(pack_kernel, (full, slab, slab), [VMEM], name="pack")(lines)
    before, after = both_sides(down, up, "gz")
    both = call(merge_kernel, full, [VMEM, VMEM, VMEM], name="merge")(own, before, after)
    width = BUF * LX
    before, after = both_sides(both[:, :width], both[:, CORE * LX - width :], "gy")
    both = jnp.concatenate([before, both, after], axis=1).reshape(fields, CORE, LX * LX)
    both, orbitals = lax.optimization_barrier((both, orbitals))
    before, after = both_sides(both[:, :BUF], both[:, CORE - BUF :], "gx")
    brought, wide_occ = bring_orbitals(occupations, orbitals)
    whole = jnp.concatenate([before, both, after], axis=1)
    return whole[0], whole[1], brought, wide_occ


def exchange(value, axis, rows):
    parts = value.shape[0] // rows
    tile = math.gcd(rows, 8)
    shaped = value.reshape(value.shape[0] // tile, tile, LANES)
    return lax.all_to_all(shaped, axis, split_axis=0, concat_axis=0, tiled=True).reshape(
        value.shape
    )


def on_device(orbitals, potential, ion_potential, occupations):
    pot_ext, ion_ext, brought, wide_occ = refill(
        potential, ion_potential, orbitals, occupations
    )
    new_orbitals, send = filtered_set(wide_occ, brought, pot_ext)
    got = exchange(send, "gy", KEPT * KEPT // PER)
    send = along_y(got)
    got = exchange(send, ("gx", "gz"), CHUNK)
    send = on_plane(got)
    got = exchange(send, ("gx", "gz"), 6)
    send, density, base = on_window(got, ion_ext)
    got = exchange(send, "gy", LANES)
    new_potential = last_step(got, base)
    return (new_orbitals, density, new_potential)


def solution(mesh):
    placed = (P(None, "gx", ("gy", "gz")), P("gx", "gy", "gz"), P("gx", "gy", "gz"), P())
    return jax.shard_map(
        on_device,
        mesh=mesh,
        in_specs=placed,
        out_specs=(P(None, "gx", ("gy", "gz")), P("gx", "gy", "gz"), P("gx", ("gy", "gz"))),
        check_vma=False,
    )
```

```python
import functools
import math

import jax
import jax.numpy as jnp
import numpy as np
from jax import lax
from jax.experimental import pallas as pl
from jax.experimental.pallas import tpu as pltpu
from jax.sharding import PartitionSpec as P

BUF = 8
DEGREE = 10
N = 128
CORE = 16
LX = 32
NORB = 8
PARTS = 8
FIRST, LAST = 4, 28
KEPT = LAST - FIRST
LANES = 128
CHUNK = 7
GROUP = 32
PER = LANES // LX

spacing = 0.2
kinetic = 0.5 / (spacing * spacing)
filter_low = 6.0
filter_high = 12.0 * kinetic
centre_value = 0.5 * (filter_low + filter_high)
half_width = 0.5 * (filter_high - filter_low)

F32, BF16 = jnp.float32, jnp.bfloat16
VMEM = pl.BlockSpec(memory_space=pltpu.VMEM)
SMEM = pl.BlockSpec(memory_space=pltpu.SMEM)
INTERPRET = False


def call(kernel, out_shape, in_specs, scratch=(), flops=1000000, name=None):
    many = isinstance(out_shape, (tuple, list))
    return pl.pallas_call(
        kernel,
        out_shape=out_shape,
        in_specs=in_specs,
        out_specs=tuple(VMEM for _ in out_shape) if many else VMEM,
        scratch_shapes=scratch,
        compiler_params=pltpu.CompilerParams(vmem_limit_bytes=40 * 1024 * 1024),
        cost_estimate=pl.CostEstimate(flops=flops, bytes_accessed=1000000, transcendentals=0),
        interpret=INTERPRET,
        name=name,
    )


def _basis():
    n = np.arange(N, dtype=np.float64)
    angle = 2.0 * np.pi * np.mod(np.outer(n, n), N) / N
    return (np.cos(angle) + np.sin(angle)) / math.sqrt(N)


def _pair(table):
    high = np.asarray(table, np.float32).astype(jnp.bfloat16)
    low = (np.asarray(table, np.float64) - high.astype(np.float64)).astype(jnp.bfloat16)
    return high, low


def _cell(part, a):
    return np.mod(CORE * part + a - BUF, N)


def _tables():
    basis = _basis()
    parts = np.arange(PARTS)
    along = np.zeros((PARTS, CORE + LX, PARTS * KEPT))
    for i in range(PARTS):
        for other in range(PARTS):
            for xx in range(KEPT):
                column = other * KEPT + xx
                cell = _cell(other, xx + FIRST)
                along[i, :CORE, column] = basis[CORE * i : CORE * (i + 1), cell]
                for a in range(LX):
                    if _cell(i, a) == cell and min((other - i) % PARTS, (i - other) % PARTS) <= 1:
                        along[i, CORE + (a % 2) * CORE + a // 2, column] = 1.0
    lane = np.arange(PARTS * LANES)
    z_cell = _cell(lane // LANES, lane % LX)
    z_table = basis[z_cell, :]
    y_lo, y_hi, j = np.meshgrid(np.arange(PER), np.arange(KEPT // PER), parts, indexing="ij")
    y_table = basis[:, _cell(j, FIRST + PER * y_hi + y_lo).reshape(-1)]
    back = np.zeros((4, 64, N))
    for q in range(4):
        y_lo, y_half, j = np.meshgrid(np.arange(PER), np.arange(2), parts, indexing="ij")
        back[q] = basis[_cell(j, 8 * q + PER * y_half + y_lo).reshape(-1), :]
    last = np.stack([basis[_cell(i, np.arange(LX)), :] for i in range(PARTS)])
    wave = 4.0 / (spacing * spacing) * np.sin(np.pi * np.arange(N) / N) ** 2
    return dict(
        along=_pair(along),
        z_table=_pair(z_table),
        z_back=_pair(z_table.T),
        y_table=_pair(y_table),
        y_back=_pair(back),
        last=_pair(last),
        wave=np.repeat(wave.astype(np.float32)[:, None], LANES, axis=1),
        wave_yz=(wave[:, None] + wave[None, :]).astype(np.float32),
    )


def _weight():
    position = np.arange(LX, dtype=np.float32)
    rising = np.clip((position + 0.5 - 0.5 * BUF) / BUF, 0.0, 1.0)
    falling = np.clip((LX - 0.5 * BUF - 0.5 - position) / BUF, 0.0, 1.0)
    profile = (rising * falling).astype(np.float32)
    return profile[:, None] * (profile[:, None] * profile[None, :]).reshape(1, LX * LX)


TABLES = _tables()
WEIGHT = _weight().astype(np.float32)


def halves(value):
    high = value.astype(BF16)
    return high, (value - high.astype(F32)).astype(BF16)


def dot3(left, right):
    def one(a, b):
        return jnp.dot(a, b, preferred_element_type=F32)

    return one(left[0], right[0]) + (one(left[0], right[1]) + one(left[1], right[0]))


def iota(shape, dim):
    return lax.broadcasted_iota(jnp.int32, shape, dim)


def swap_four(v, lane):
    low, even = lane < 2 * LX, (lane // LX) % 2 == 0
    w = [None] * 4
    for g in range(2):
        w[g] = jnp.where(low, v[g], pltpu.roll(v[g + 2], 2 * LX, 1))
        w[g + 2] = jnp.where(low, pltpu.roll(v[g], 2 * LX, 1), v[g + 2])
    out = []
    for g in (0, 2):
        out.append(jnp.where(even, w[g], pltpu.roll(w[g + 1], LX, 1)))
        out.append(jnp.where(even, pltpu.roll(w[g], 3 * LX, 1), w[g + 1]))
    return out


def swap_inner(v, row, lane):
    a, b = row % 4, lane // LX
    turned = pltpu.roll(v, 2 * LX, 1)
    v = jnp.where(
        a // 2 == b // 2,
        v,
        jnp.where(a < 2, pltpu.roll(turned, 6, 0), pltpu.roll(turned, 2, 0)),
    )
    return jnp.where(
        a % 2 == b % 2,
        v,
        jnp.where(
            a % 2 == 0,
            pltpu.roll(pltpu.roll(v, LX, 1), 7, 0),
            pltpu.roll(pltpu.roll(v, 3 * LX, 1), 1, 0),
        ),
    )


def bring_kernel(occ_ref, orb_ref, out_ref, wide_ref):
    tiles, chunks = LX // 8, LX * LX // LANES
    lane = iota((8, LANES), 1)
    line = LX + 2
    for n in range(NORB):
        wide_ref[n : n + 1, :] = jnp.full((1, LANES), occ_ref[n], F32)
    for h in range(2):
        out_ref[h * line] = jnp.zeros((LX, LANES), F32)
        out_ref[h * line + line - 1] = jnp.zeros((LX, LANES), F32)

    def bring(c, carry):
        here = pl.ds(pl.multiple_of(c * LANES, LANES), LANES)
        for t in range(tiles):
            rows = slice(8 * t, 8 * t + 8)
            for h in range(2):
                v = [orb_ref[4 * h + g, rows, here].astype(F32) for g in range(4)]
                for y, value in enumerate(swap_four(v, lane)):
                    out_ref[h * line + 1 + PER * c + y, rows, :] = value
        return carry

    lax.fori_loop(0, chunks, bring, 0)


def bring_orbitals(occupations, orbitals):
    return call(
        bring_kernel,
        (
            jax.ShapeDtypeStruct((2 * (LX + 2), LX, LANES), F32),
            jax.ShapeDtypeStruct((NORB, LANES), F32),
        ),
        [SMEM, VMEM],
        flops=15000000,
        name="bring",
    )(occupations, orbitals)


def filter_kernel(occ_ref, orb_ref, pot_ref, weight_ref, new_ref, send_ref, ya, yb, coef, flat):
    tiles, chunks = LX // 8, LX * LX // LANES
    line = LX + 2
    lane = iota((8, LANES), 1)
    row = iota((8, LANES), 0)
    low_z, high_z = lane % LX == 0, lane % LX == LX - 1
    first_x, last_x = row == 0, row == 7
    zero = jnp.zeros((8, LANES), F32)
    alpha = -2.0 * kinetic / half_width
    scale, shift = 2.0 / half_width, (2.0 / half_width) * (6.0 * kinetic - centre_value)

    for buffer in (ya, yb):
        for h in range(2):
            buffer[h * line] = jnp.zeros((LX, LANES), F32)
            buffer[h * line + line - 1] = jnp.zeros((LX, LANES), F32)

    def spread(c, carry):
        here = pl.ds(pl.multiple_of(c * LANES, LANES), LANES)
        for t in range(tiles):
            rows = slice(8 * t, 8 * t + 8)
            v = scale * pot_ref[rows, here] + shift
            for y in range(PER):
                value = jnp.where(lane // LX == y, v, 0.0)
                value = value + pltpu.roll(value, LX, 1)
                coef[PER * c + y, rows, :] = value + pltpu.roll(value, 2 * LX, 1)
        return carry

    lax.fori_loop(0, chunks, spread, 0)

    def advance(src, before, dst):
        def one(b, carry):
            for yy in range(GROUP):
                y = GROUP * b + yy
                for h in range(2):
                    at = h * line + 1 + y
                    cells = [src[at, 8 * t : 8 * t + 8, :] for t in range(tiles)]
                    for t in range(tiles):
                        rows = slice(8 * t, 8 * t + 8)
                        cur = cells[t]
                        above = cells[t - 1] if t > 0 else zero
                        below = cells[t + 1] if t < tiles - 1 else zero
                        total = jnp.where(low_z, zero, pltpu.roll(cur, 1, 1))
                        total += jnp.where(high_z, zero, pltpu.roll(cur, LANES - 1, 1))
                        total += pltpu.roll(jnp.where(last_x, above, cur), 1, 0)
                        total += pltpu.roll(jnp.where(first_x, below, cur), 7, 0)
                        total += src[at - 1, rows, :] + src[at + 1, rows, :]
                        result = alpha * total + coef[y, rows, :] * cur
                        if before is None:
                            dst[at, rows, :] = 0.5 * result
                        else:
                            dst[at, rows, :] = result - before[at, rows, :]
            return carry

        lax.fori_loop(0, LX // GROUP, one, 0)

    advance(orb_ref, None, yb)
    advance(yb, orb_ref, ya)

    def two(m, carry):
        advance(ya, yb, yb)
        advance(yb, ya, ya)
        return carry

    lax.fori_loop(0, (DEGREE - 2) // 2, two, 0)

    pairs = [(n, m) for n in range(NORB) for m in range(n + 1)]

    def take(c, carry):
        here = pl.ds(pl.multiple_of(c * LANES, LANES), LANES)
        for t in range(tiles):
            rows = slice(8 * t, 8 * t + 8)
            for h in range(2):
                v = [ya[h * line + 1 + PER * c + y, rows, :] for y in range(PER)]
                for g, value in enumerate(swap_four(v, lane)):
                    flat[4 * h + g, rows, here] = value
        return carry

    lax.fori_loop(0, chunks, take, 0)

    def gather(t, sums):
        sums = list(sums)
        rows = pl.ds(pl.multiple_of(8 * t, 8), 8)
        for c in range(chunks):
            f = [flat[n, rows, c * LANES : (c + 1) * LANES] for n in range(NORB)]
            for at, (n, m) in enumerate(pairs):
                sums[at] = sums[at] + f[n] * f[m]
        return tuple(sums)

    sums = lax.fori_loop(0, tiles, gather, tuple(zero for _ in pairs))
    gram = {
        pair: jnp.sum(jnp.sum(s, axis=0, keepdims=True), axis=1, keepdims=True) / float(LX**3)
        for pair, s in zip(pairs, sums)
    }
    factor, inverse, recip = {}, {}, {}
    for j in range(NORB):
        rest = gram[j, j]
        for k in range(j):
            rest = rest - factor[j, k] * factor[j, k]
        recip[j] = 1.0 / jnp.sqrt(rest)
        for n in range(j + 1, NORB):
            value = gram[n, j]
            for k in range(j):
                value = value - factor[n, k] * factor[j, k]
            factor[n, j] = value * recip[j]
    for j in range(NORB):
        inverse[j, j] = recip[j]
        for n in range(j + 1, NORB):
            value = factor[n, j] * inverse[j, j]
            for k in range(j + 1, n):
                value = value + factor[n, k] * inverse[k, j]
            inverse[n, j] = -recip[n] * value
    wide = {pair: jnp.broadcast_to(inverse[pair], (8, LANES)) for pair in pairs}

    kept = KEPT // PER
    occ = [jnp.broadcast_to(occ_ref[n : n + 1, :], (8, LANES)) for n in range(NORB)]

    def normal(t, carry):
        rows = pl.ds(pl.multiple_of(8 * t, 8), 8)
        for c in range(chunks):
            here = slice(c * LANES, (c + 1) * LANES)
            f = [flat[n, rows, here] for n in range(NORB)]
            total = zero
            for n in range(NORB):
                value = wide[n, 0] * f[0]
                for m in range(1, n + 1):
                    value = value + wide[n, m] * f[m]
                flat[n, rows, here] = value
                total = total + occ[n] * (value * value)
            if 1 <= c <= kept:
                coef[c, rows, :] = swap_inner(total * weight_ref[rows, here], row, lane)
        return carry

    lax.fori_loop(0, tiles, normal, 0)

    def finish(n, carry):
        new_ref[n] = flat[n].astype(BF16)
        return carry

    lax.fori_loop(0, NORB, finish, 0)

    for c in range(kept):
        for x in range(kept):
            value = coef[c + 1, PER * (x + 1) : PER * (x + 2), :]
            for s in range(PARTS):
                start = s * KEPT * kept + PER * c * kept + x
                send_ref[pl.ds(start, PER, stride=kept), :] = value


def filtered_set(occupations, orbitals, potential_ext):
    return call(
        filter_kernel,
        (
            jax.ShapeDtypeStruct((NORB, LX, LX * LX), BF16),
            jax.ShapeDtypeStruct((PARTS * KEPT * KEPT // PER, LANES), F32),
        ),
        [VMEM, VMEM, VMEM, VMEM],
        [
            pltpu.VMEM((2 * (LX + 2), LX, LANES), F32),
            pltpu.VMEM((2 * (LX + 2), LX, LANES), F32),
            pltpu.VMEM((LX, LX, LANES), F32),
            pltpu.VMEM((NORB, LX, LX * LX), F32),
        ],
        flops=60000000,
        name="filter",
    )(occupations, orbitals, potential_ext, jnp.asarray(WEIGHT))


def crop(value, lane):
    out = pltpu.roll(value, LANES - FIRST, 1)
    for x in range(1, PER):
        moved = pltpu.roll(value, LANES - FIRST - 8 * x, 1)
        out = jnp.where(lane < KEPT * x, out, moved)
    return out


def uncrop(value, lane):
    out = jnp.zeros_like(value)
    inside = (lane % LX >= FIRST) & (lane % LX < LAST)
    for x in range(PER):
        here = inside & (lane // LX == x)
        out = jnp.where(here, pltpu.roll(value, FIRST + 8 * x, 1), out)
    return out


def y_kernel(got_ref, high_ref, low_ref, send_ref):
    kept = KEPT // PER
    part = kept // 2
    at = lax.axis_index("gy")
    odd = lax.rem(lax.axis_index("gx"), 2) == 1
    lane = iota((CORE, LANES), 1)
    table = (high_ref[at], low_ref[at])
    waves, folded = [], ([], [])
    for c in range(kept):
        lines = got_ref[pl.ds(c, PARTS * KEPT, stride=kept), :]
        value = dot3(table, halves(lines))
        waves.append(crop(value[:CORE], lane))
        for s in range(2):
            folded[s].append(crop(value[CORE * (1 + s) : CORE * (2 + s)], lane))
    for q in range(4):
        planes = folded[q // 2]
        thirds = []
        for c in range(part):
            low, high = planes[c], planes[part + c]
            first, second = (low, high) if q % 2 == 0 else (high, low)
            thirds.append(jnp.where(odd, second, first))
        for c in range(kept):
            piece = pltpu.roll(thirds[1 + c // part], 3 * LX - LX * (c % part), 1)
            row = jnp.where(lane < 3 * LX, waves[c], piece)
            send_ref[pl.ds(q * CHUNK + c, CORE, stride=4 * CHUNK), :] = row
        send_ref[pl.ds(q * CHUNK + kept, CORE, stride=4 * CHUNK), :] = thirds[0]


def along_y(got):
    return call(
        y_kernel,
        jax.ShapeDtypeStruct((64 * CHUNK, LANES), F32),
        [VMEM, VMEM, VMEM],
        name="along_y",
    )(got, *map(jnp.asarray, TABLES["along"]))


def plane_kernel(
    got_ref,
    zh_ref,
    zl_ref,
    yh_ref,
    yl_ref,
    wave_ref,
    own_ref,
    bh_ref,
    bl_ref,
    th_ref,
    tl_ref,
    send_ref,
):
    kept = KEPT // PER
    part = kept // 2
    out_chunk = 6
    wide = PARTS * LANES
    lane = iota((PARTS, LANES), 1)
    blocks, thirds = [], []
    for k in range(PARTS):
        rows = [got_ref[pl.ds(CHUNK * k + c, PARTS, stride=CHUNK * PARTS), :] for c in range(CHUNK)]
        blocks.append(jnp.concatenate([uncrop(rows[c], lane) for c in range(kept)], axis=0))
        units = [rows[kept]]
        for u in range(2):
            unit = pltpu.roll(rows[part * u], LX, 1)
            for c in range(1, part):
                moved = pltpu.roll(rows[part * u + c], LX + LX * c, 1)
                unit = jnp.where(lane < LX * c, unit, moved)
            units.append(unit)
        thirds.append([uncrop(unit, lane) for unit in units])
    lines = jnp.concatenate(blocks, axis=1)
    which = (iota(lines.shape, 1) % LANES) // LX
    spread = jnp.concatenate([jnp.where(which == y, lines, 0.0) for y in range(PER)], axis=0)
    along_z = dot3(halves(spread), (zh_ref[...], zl_ref[...]))
    spectrum = dot3((yh_ref[...], yl_ref[...]), halves(along_z))
    member = lax.axis_index("gx") * PARTS + lax.axis_index("gz")
    number = lax.axis_index("gy") * CORE + lax.div(member, 4)
    eigen = wave_ref[...] + own_ref[pl.ds(number, 1), :]
    positive = eigen > 0.0
    green = jnp.where(positive, 4.0 * math.pi / jnp.where(positive, eigen, 1.0), 0.0)
    spectrum = spectrum * green
    quarter = lax.rem(member, 4)
    lines = dot3((bh_ref[quarter], bl_ref[quarter]), halves(spectrum))
    spread = dot3(halves(lines), (th_ref[...], tl_ref[...]))
    which = (iota((16, wide), 1) % LANES) // LX
    packed = jnp.zeros((16, wide), F32)
    for y in range(PER):
        packed = jnp.where(which == y, spread[16 * y : 16 * (y + 1)], packed)
    for k in range(PARTS):
        for half in range(2):
            send_ref[pl.ds(out_chunk * k + half, PARTS, stride=out_chunk * PARTS), :] = packed[
                8 * half : 8 * half + 8, k * LANES : (k + 1) * LANES
            ]
    left = lane % LX < LX // 2
    half = LX // 2
    own = iota((PARTS, LANES), 0) % 2 == lax.rem(member, 2)
    for h in range(4):
        line = []
        for k in range(PARTS):
            if h == 0:
                line.append(pltpu.roll(thirds[k][0], 1, 0))
            elif h == part:
                line.append(thirds[k][part - 1])
            else:
                line.append(thirds[k][h - 1] + pltpu.roll(thirds[k][h], 1, 0))
        for k in range(PARTS):
            beside = jnp.where(left, line[(k + 1) % PARTS], line[(k - 1) % PARTS])
            value = line[k] + jnp.where(
                left, pltpu.roll(beside, LANES - half, 1), pltpu.roll(beside, half, 1)
            )
            value = jnp.where(own, value, pltpu.roll(value, PARTS - 1, 0))
            send_ref[pl.ds(out_chunk * k + 2 + h, PARTS, stride=out_chunk * PARTS), :] = value


def on_plane(got):
    t = TABLES
    return call(
        plane_kernel,
        jax.ShapeDtypeStruct((64 * 6, LANES), F32),
        [VMEM] * 11,
        name="on_plane",
    )(
        got,
        *map(jnp.asarray, t["z_table"]),
        *map(jnp.asarray, t["y_table"]),
        jnp.asarray(t["wave_yz"]),
        jnp.asarray(t["wave"]),
        *map(jnp.asarray, t["y_back"]),
        *map(jnp.asarray, t["z_back"]),
    )


def cube_root(value):
    safe = jnp.maximum(value, 1e-30)
    root = jnp.exp(jnp.log(safe) * (1.0 / 3.0))
    root = root - (root - safe / (root * root)) * (1.0 / 3.0)
    return jnp.where(value > 0.0, root, 0.0)


def exchange_correlation(density):
    root = cube_root(density)
    slater = -((3.0 / math.pi) ** (1.0 / 3.0)) * root
    radius = (3.0 / (4.0 * math.pi)) ** (1.0 / 3.0)
    bottom = radius + 7.8 * root
    wigner = -0.44 * root / bottom * (1.0 + radius / (3.0 * bottom))
    return slater + wigner


def window_kernel(got_ref, ion_ref, send_ref, dens_ref, base_ref, work):
    for half in range(2):
        value = got_ref[pl.ds(half, 64, stride=6), :]
        for s in range(PARTS):
            send_ref[pl.ds(s * LANES + half, 64, stride=2), :] = value
    row, lane = iota((8, LANES), 0), iota((8, LANES), 1)
    odd = lax.rem(lax.axis_index("gx"), 2) == 1
    for q in range(2):
        for h in range(4):
            x = 4 * q + h
            value = jnp.where(
                odd,
                got_ref[pl.ds(6 * (1 - q) + 2 + h, LX, stride=12), :],
                got_ref[pl.ds(6 * q + 2 + h, LX, stride=12), :],
            )
            if 2 <= x < 6:
                for low in range(PER):
                    core = pltpu.roll(value[BUF : BUF + CORE], LANES - LX * low - BUF, 1)
                    dens_ref[PER * (x - 2) + low] = core[:, :CORE]
            for t in range(4):
                piece = swap_inner(value[8 * t : 8 * t + 8], row, lane)
                for half in range(2):
                    y = 2 * t + half
                    work[PER * x : PER * x + PER, y * LANES : (y + 1) * LANES] = piece[
                        PER * half : PER * half + PER
                    ]
    base_ref[...] = ion_ref[...] + exchange_correlation(work[...])


def on_window(got, ion_ext):
    return call(
        window_kernel,
        (
            jax.ShapeDtypeStruct((PARTS * LANES, LANES), F32),
            jax.ShapeDtypeStruct((CORE, CORE, CORE), F32),
            jax.ShapeDtypeStruct((LX, LX * LX), F32),
        ),
        [VMEM, VMEM],
        [pltpu.VMEM((LX, LX * LX), F32)],
        name="on_window",
    )(got, ion_ext)


def last_kernel(got_ref, base_ref, high_ref, low_ref, out_ref):
    at = lax.axis_index("gy")
    table = (high_ref[at], low_ref[at])
    row, lane = iota((8, LANES), 0), iota((8, LANES), 1)
    for x in range(8):
        lines = got_ref[pl.ds(x, N, stride=8), :]
        value = dot3(table, halves(lines))
        rows = slice(PER * x, PER * x + PER)
        for t in range(4):
            piece = swap_inner(value[8 * t : 8 * t + 8], row, lane)
            for half in range(2):
                y = 2 * t + half
                here = slice(y * LANES, (y + 1) * LANES)
                out_ref[rows, here] = base_ref[rows, here] + piece[PER * half : PER * half + PER]


def last_step(got, base):
    return call(
        last_kernel,
        jax.ShapeDtypeStruct((LX, LX * LX), F32),
        [VMEM, VMEM, VMEM, VMEM],
        name="last_step",
    )(got, base, *map(jnp.asarray, TABLES["last"]))


def both_sides(first, last, axis):
    count = lax.axis_size(axis)
    up = [(i, (i + 1) % count) for i in range(count)]
    down = [(j, i) for i, j in up]
    return lax.ppermute(last, axis, up), lax.ppermute(first, axis, down)


def pack_kernel(fields_ref, own_ref, up_ref, down_ref):
    lane = iota((CORE, LANES), 1)
    third = (lane % LX) // BUF
    for f in range(2):
        rows = slice(CORE * f, CORE * (f + 1))
        up, down = jnp.zeros((CORE, LANES), F32), jnp.zeros((CORE, LANES), F32)
        for c in range(PER):
            value = jnp.zeros((CORE, LANES), F32)
            for y in range(PER):
                line = fields_ref[pl.ds(f * CORE * CORE + PER * c + y, CORE, stride=CORE), :]
                line = jnp.concatenate([line, jnp.zeros((CORE, LANES - CORE), F32)], axis=1)
                value = value + pltpu.roll(line, LX * y + BUF, 1)
            own_ref[rows, c * LANES : (c + 1) * LANES] = value
            up = jnp.where(third == c, pltpu.roll(value, (BUF * c - 2 * BUF) % LANES, 1), up)
            down = jnp.where(third == c, pltpu.roll(value, (BUF * c - BUF) % LANES, 1), down)
        up_ref[rows, :] = up
        down_ref[rows, :] = down


def merge_kernel(own_ref, before_ref, after_ref, out_ref):
    third = (iota((2 * CORE, LANES), 1) % LX) // BUF
    before, after = before_ref[...], after_ref[...]
    for c in range(PER):
        here = slice(c * LANES, (c + 1) * LANES)
        value = jnp.where(third == 0, pltpu.roll(before, (-BUF * c) % LANES, 1), own_ref[:, here])
        out_ref[:, here] = jnp.where(
            third == 3, pltpu.roll(after, (3 * BUF - BUF * c) % LANES, 1), value
        )


def refill(potential, ion_potential, orbitals, occupations):
    fields = 2
    count = fields * CORE
    slab = jax.ShapeDtypeStruct((count, LANES), F32)
    full = jax.ShapeDtypeStruct((count, CORE * LX), F32)
    lines = jnp.concatenate([potential, ion_potential]).reshape(fields * CORE * CORE, CORE)
    own, up, down = call(pack_kernel, (full, slab, slab), [VMEM], name="pack")(lines)
    before, after = both_sides(down, up, "gz")
    both = call(merge_kernel, full, [VMEM, VMEM, VMEM], name="merge")(own, before, after)
    width = BUF * LX
    before, after = both_sides(both[:, :width], both[:, CORE * LX - width :], "gy")
    both = jnp.concatenate([before, both, after], axis=1).reshape(fields, CORE, LX * LX)
    both, orbitals = lax.optimization_barrier((both, orbitals))
    before, after = both_sides(both[:, :BUF], both[:, CORE - BUF :], "gx")
    brought, wide_occ = bring_orbitals(occupations, orbitals)
    whole = jnp.concatenate([before, both, after], axis=1)
    return whole[0], whole[1], brought, wide_occ


def exchange(value, axis, rows):
    parts = value.shape[0] // rows
    tile = math.gcd(rows, 8)
    shaped = value.reshape(value.shape[0] // tile, tile, LANES)
    return lax.all_to_all(shaped, axis, split_axis=0, concat_axis=0, tiled=True).reshape(
        value.shape
    )


def on_device(orbitals, potential, ion_potential, occupations):
    pot_ext, ion_ext, brought, wide_occ = refill(
        potential, ion_potential, orbitals, occupations
    )
    new_orbitals, send = filtered_set(wide_occ, brought, pot_ext)
    got = exchange(send, "gy", KEPT * KEPT // PER)
    send = along_y(got)
    got = exchange(send, ("gx", "gz"), CHUNK)
    send = on_plane(got)
    got = exchange(send, ("gx", "gz"), 6)
    send, density, base = on_window(got, ion_ext)
    got = exchange(send, "gy", LANES)
    new_potential = last_step(got, base)
    return (new_orbitals, density, new_potential)


def solution(mesh):
    placed = (P(None, "gx", ("gy", "gz")), P("gx", "gy", "gz"), P("gx", "gy", "gz"), P())
    return jax.shard_map(
        on_device,
        mesh=mesh,
        in_specs=placed,
        out_specs=(P(None, "gx", ("gy", "gz")), P("gx", "gy", "gz"), P("gx", ("gy", "gz"))),
        check_vma=False,
    )
```
